32 devices in a mesh: batch: 4 (over y, z), dap: 8 (over x, core).
Axes of the slice: x: 4, y: 2, z: 2, core: 2. Of those that a mesh axis runs over, the one named last changes fastest.
The devices are a block of a 4x4x8 slice.
Arguments:
- z_pair: bfloat16 [1024, 256, 128], P(('batch', 'dap')), parts along dimension 0
- msa_feat: bfloat16 [512, 1024, 64], P(None, ('batch', 'dap')), parts along dimension 1
- ln_scale: bfloat16 [64], replicated
- ln_offset: bfloat16 [64], replicated
- w_a: bfloat16 [64, 32], replicated
- b_a: bfloat16 [32], replicated
- w_b: bfloat16 [64, 32], replicated
- b_b: bfloat16 [32], replicated
- w_out: bfloat16 [1024, 128], replicated
- b_out: bfloat16 [128], replicated
Outputs:
- output: bfloat16 [1024, 256, 128], P(('batch', 'dap')), parts along dimension 0
There are 4 independent parts. The reference program is written for one: setup_inputs(seed, part) draws one part's arguments, and reference() takes and returns one part's arrays. A program takes and returns all parts, laid end to end along the dimension named above; an argument that names none is the same for every part.
All inputs are finite; a program needn't handle non-finite values.
Results may differ from the reference program's by a relative error of at most 0.001.
Values are sent between devices in bfloat16 or wider.
A program may use at most 768 MiB of HBM per device.

```python
import jax
import jax.numpy as jnp
from jax import lax

MSA_ROWS = 512
N_RES = 256
MSA_DIM = 64
HID_DIM = 32
PAIR_DIM = 128
LOW_RANK = 4

LN_EPS = 1e-5
ROW_TILE = min(N_RES, max(1, 8192 // N_RES))


def normal_draw(rng_key, shape_in, scale_in):
    return jax.random.normal(rng_key, shape_in, jnp.float32) * scale_in


def setup_inputs(seed: int = 0, part: int = 0) -> dict:
    part_keys = jax.random.split(jax.random.fold_in(jax.random.key(seed), part), 4)
    shared_keys = jax.random.split(jax.random.key(seed + 1), 8)
    mix_coef = normal_draw(part_keys[0], (MSA_ROWS, LOW_RANK), 1.0)
    res_feat = normal_draw(part_keys[1], (LOW_RANK, N_RES, MSA_DIM), 1.0)
    msa_noise = normal_draw(part_keys[2], (MSA_ROWS, N_RES, MSA_DIM), 0.5)
    msa_f32 = jnp.einsum('sr,rnm->snm', mix_coef, res_feat) * LOW_RANK ** -0.5 + msa_noise
    z_f32 = normal_draw(part_keys[3], (N_RES, N_RES, PAIR_DIM), 1.0)
    return {
        'z_pair': z_f32.astype(jnp.bfloat16),
        'msa_feat': msa_f32.astype(jnp.bfloat16),
        'ln_scale': (1.0 + normal_draw(shared_keys[0], (MSA_DIM,), 0.5)).astype(jnp.bfloat16),
        'ln_offset': normal_draw(shared_keys[1], (MSA_DIM,), 0.5).astype(jnp.bfloat16),
        'w_a': normal_draw(shared_keys[2], (MSA_DIM, HID_DIM), MSA_DIM ** -0.5).astype(jnp.bfloat16),
        'b_a': normal_draw(shared_keys[3], (HID_DIM,), 0.5).astype(jnp.bfloat16),
        'w_b': normal_draw(shared_keys[4], (MSA_DIM, HID_DIM), MSA_DIM ** -0.5).astype(jnp.bfloat16),
        'b_b': normal_draw(shared_keys[5], (HID_DIM,), 0.5).astype(jnp.bfloat16),
        'w_out': normal_draw(shared_keys[6], (HID_DIM * HID_DIM, PAIR_DIM), (HID_DIM * HID_DIM) ** -0.5).astype(jnp.bfloat16),
        'b_out': normal_draw(shared_keys[7], (PAIR_DIM,), 0.5).astype(jnp.bfloat16),
    }


def layer_norm(msa_feat, ln_scale, ln_offset):
    msa_f32 = msa_feat.astype(jnp.float32)
    mean_val = jnp.mean(msa_f32, axis=-1, keepdims=True)
    centred = msa_f32 - mean_val
    var_val = jnp.mean(centred * centred, axis=-1, keepdims=True)
    normed = centred / jnp.sqrt(var_val + LN_EPS)
    return (normed * ln_scale.astype(jnp.float32) + ln_offset.astype(jnp.float32)).astype(jnp.bfloat16)


def project(msa_norm, weight, bias_vec):
    flat_rows = msa_norm.reshape(-1, msa_norm.shape[-1])
    out_f32 = jnp.dot(flat_rows, weight, preferred_element_type=jnp.float32) + bias_vec.astype(jnp.float32)
    return out_f32.astype(jnp.bfloat16).reshape(msa_norm.shape[0], msa_norm.shape[1], weight.shape[1])


def reference(z_pair, msa_feat, ln_scale, ln_offset, w_a, b_a, w_b, b_b, w_out, b_out):
    msa_norm = layer_norm(msa_feat, ln_scale, ln_offset)
    proj_a = project(msa_norm, w_a, b_a).astype(jnp.float32)
    proj_b = project(msa_norm, w_b, b_b).astype(jnp.float32)
    w_cube = w_out.astype(jnp.float32).reshape(HID_DIM, HID_DIM, PAIR_DIM)
    bias_out = b_out.astype(jnp.float32)
    inv_seq = 1.0 / MSA_ROWS

    def tile_fn(tile_idx):
        row_start = tile_idx * ROW_TILE
        a_tile = lax.dynamic_slice_in_dim(proj_a, row_start, ROW_TILE, axis=1)
        z_tile = lax.dynamic_slice_in_dim(z_pair, row_start, ROW_TILE, axis=0)
        outer_prod = jnp.einsum('sic,sjd->icjd', a_tile, proj_b) * inv_seq
        outer_prod = outer_prod.astype(jnp.bfloat16).astype(jnp.float32)
        update = jnp.einsum('icjd,cdz->ijz', outer_prod, w_cube) + bias_out
        return (z_tile.astype(jnp.float32) + update).astype(jnp.bfloat16)

    row_tiles = lax.map(tile_fn, jnp.arange(N_RES // ROW_TILE))
    return row_tiles.reshape(N_RES, N_RES, PAIR_DIM)
```

```python
import functools

import jax
import jax.numpy as jnp
from jax import lax
from jax.experimental import pallas as pl
from jax.experimental.pallas import tpu as pltpu
from jax.sharding import PartitionSpec as P

LN_EPS = 1e-5
F32 = jnp.float32
BF16 = jnp.bfloat16
LANES = 128
HALF = 16
PIECES = 4
MESH = pl.DeviceIdType.MESH


def iota(shape, dim):
    return lax.broadcasted_iota(jnp.int32, shape, dim)


def column_lanes(row, count):
    spread = jnp.broadcast_to(row, (count, count))
    picked = jnp.where(iota((count, count), 0) == iota((count, count), 1), spread, 0.0)
    return jnp.broadcast_to(jnp.sum(picked, axis=1, keepdims=True), (count, LANES))


def kernel(n_dev, z_hbm, x_hbm, ls_hbm, lo_hbm, wa_hbm, ba_hbm, wb_hbm, bb_hbm, wo_hbm, bo_hbm, out_hbm,
           z_buf, x_buf, ls_v, lo_v, wa_v, ba_v, wb_v, bb_v, wo_v, bo_v,
           scale_bc, offset_bc, bias_a, bias_b, row_bc, proj_a_w, proj_b_w, a_mat, bt, o_mat, w_f32, w_diag, u_acc,
           small_sem, x_sem, z_sem, out_sem, recv_sem, right_sem, left_sem, sib_sem):
    n_seq = x_hbm.shape[1]
    n_loc = z_hbm.shape[0]
    m_dim = wa_hbm.shape[1]
    hid = wa_hbm.shape[0]
    inv_seq = 1.0 / n_seq
    me = lax.axis_index('dap')
    core = lax.rem(me, 2)
    sib = me + 1 - 2 * core
    right = lax.rem(me + 2, n_dev)
    left = lax.rem(me + n_dev - 2, n_dev)

    barrier = pltpu.get_barrier_semaphore()
    for peer in (sib, right, left):
        pl.semaphore_signal(barrier, inc=1, device_id={'dap': peer}, device_id_type=MESH)

    small = [pltpu.make_async_copy(src, dst, small_sem.at[k]) for k, (src, dst) in enumerate((
        (wb_hbm, wb_v), (bb_hbm, bb_v), (ls_hbm, ls_v), (lo_hbm, lo_v), (wa_hbm, wa_v), (ba_hbm, ba_v),
        (wo_hbm, wo_v), (bo_hbm, bo_v)))]
    x_rows = 4 * m_dim
    x_copies = [pltpu.make_async_copy(x_hbm.at[pl.ds(k * x_rows, x_rows)], x_buf.at[pl.ds(k * x_rows, x_rows)], x_sem.at[k])
                for k in range(n_loc // 4)]
    for copy in small[:4]:
        copy.start()
    for copy in x_copies[:4]:
        copy.start()
    for copy in small[4:6]:
        copy.start()
    for copy in x_copies[4:]:
        copy.start()
    for copy in small[6:]:
        copy.start()
    z_copy = pltpu.make_async_copy(z_hbm, z_buf, z_sem)
    z_copy.start()

    for copy in small[:4]:
        copy.wait()
    row_bc[...] = column_lanes(bb_v[...].astype(F32).reshape(1, hid), hid)
    wb_rows = wb_v[...].astype(F32)
    wb_two = jnp.concatenate([wb_rows, wb_rows], axis=1)
    scale_bc[...] = column_lanes(ls_v[...].astype(F32).reshape(1, m_dim), m_dim)
    offset_bc[...] = column_lanes(lo_v[...].astype(F32).reshape(1, m_dim), m_dim)
    in_half = iota((HALF, LANES), 0)
    in_pair = iota((HALF, LANES), 1) // m_dim
    for d in range(hid):
        spread = jnp.broadcast_to(wb_two[d:d + 1, :], (HALF, LANES))
        for t in range(HALF * m_dim // LANES):
            part = jnp.where(in_half == in_pair + 2 * t, spread, 0.0)
            proj_b_w[d * HALF:(d + 1) * HALF, t * LANES:(t + 1) * LANES] = part.astype(BF16)
        bias_b[d * HALF:(d + 1) * HALF, :] = jnp.broadcast_to(row_bc[d:d + 1, :], (HALF, LANES))

    def norm_residue(n):
        rows = pl.ds(pl.multiple_of(n * m_dim, m_dim), m_dim)
        value = x_buf[rows, :].astype(F32)
        mean = jnp.sum(value, axis=0, keepdims=True) * (1.0 / m_dim)
        centred = value - mean
        var = jnp.sum(centred * centred, axis=0, keepdims=True) * (1.0 / m_dim)
        normed = centred * lax.rsqrt(var + LN_EPS)
        lanes4 = n_seq // LANES
        scale = jnp.concatenate([scale_bc[...]] * lanes4, axis=1)
        offset = jnp.concatenate([offset_bc[...]] * lanes4, axis=1)
        x_buf[rows, :] = (normed * scale + offset).astype(BF16)

    rows_piece = HALF * hid // PIECES

    def remote(src, dst, send, recv, peer):
        return pltpu.make_async_remote_copy(src_ref=src, dst_ref=dst, send_sem=send, recv_sem=recv,
                                            device_id={'dap': peer}, device_id_type=MESH)

    def slot_of(q, r, h):
        return q * 8 + r * 2 + h

    def to_right(r, h, c):
        r_there = (r + 3) % 4
        k = (0 if r == 0 else 2) + (h if r == 0 else 0)
        return remote(bt.at[slot_of(0, r, h), c], bt.at[slot_of(0, r_there, h), c], right_sem.at[k, c],
                      recv_sem.at[slot_of(0, r_there, h), c], right)

    def to_left(r, h, c):
        r_there = (r + 1) % 4
        k = (0 if r == 0 else 2) + (h if r == 0 else 0)
        return remote(bt.at[slot_of(0, r, h), c], bt.at[slot_of(0, r_there, h), c], left_sem.at[k, c],
                      recv_sem.at[slot_of(0, r_there, h), c], left)

    def to_sib(r, h, c):
        return remote(bt.at[slot_of(0, r, h), c], bt.at[slot_of(1, r, h), c], sib_sem.at[r * 2 + h, c],
                      recv_sem.at[slot_of(1, r, h), c], sib)

    def arrived(slot, c):
        remote(bt.at[slot, c], bt.at[slot, c], sib_sem.at[0, 0], recv_sem.at[slot, c], sib).wait_recv()

    sent = []

    def send(copy):
        copy.start()
        sent.append(copy)

    bias_four = None
    for h in range(2):
        for k in range(4):
            x_copies[h * 4 + k].wait()

            def body(n, carry):
                norm_residue(n)
                return carry

            lax.fori_loop((h * 4 + k) * 4, (h * 4 + k + 1) * 4, body, 0, unroll=2)
        normed = x_buf.at[pl.ds(h * HALF * m_dim, HALF * m_dim), :]
        for c in range(PIECES):
            rows = slice(c * rows_piece, (c + 1) * rows_piece)
            res = jnp.dot(proj_b_w[rows, :], normed[...], preferred_element_type=F32)
            bias = jnp.concatenate([bias_b[rows, :]] * (n_seq // LANES), axis=1)
            bt[slot_of(0, 0, h), c] = (res + bias).astype(BF16)
        if h == 0:
            pl.semaphore_wait(barrier, 3)
        for c in range(PIECES):
            send(to_right(0, h, c))
            send(to_left(0, h, c))
            send(to_sib(0, h, c))

    for copy in small[4:]:
        copy.wait()
    row_bc[...] = column_lanes(ba_v[...].astype(F32).reshape(1, hid), hid)
    bias_a[...] = jnp.concatenate([row_bc[...]] * 4, axis=0)
    wa_rows = wa_v[...].astype(F32)
    wa_wide = jnp.concatenate([jnp.concatenate([wa_rows] * 4, axis=1)] * 4, axis=0)
    same = (iota(wa_wide.shape, 0) // hid) == (iota(wa_wide.shape, 1) // m_dim)
    proj_a_w[...] = jnp.where(same, wa_wide, 0.0).astype(BF16)
    for g in range(n_loc // 4):
        res = jnp.dot(proj_a_w[...], x_buf[g * x_rows:(g + 1) * x_rows, :], preferred_element_type=F32)
        res = res + jnp.concatenate([bias_a[...]] * (n_seq // LANES), axis=1)
        a_mat[:, g * LANES:(g + 1) * LANES] = res.T.astype(BF16)

    w_f32[...] = wo_v[...].astype(F32)
    w_diag[...] = jnp.zeros_like(w_diag)

    def spread_w(d, carry):
        block = w_f32[pl.ds(d, hid, stride=hid), :].astype(BF16)
        c = d // 8
        for k in range(4):
            row = pl.multiple_of((d - c * 8) * LANES + k * hid, hid)
            w_diag[c, pl.ds(row, hid), k * LANES:(k + 1) * LANES] = block
        return carry

    lax.fori_loop(0, hid, spread_w, 0)

    def outer_piece(slot, c):
        res = jnp.dot(bt[slot, c], a_mat[...], preferred_element_type=F32)
        res = (res * inv_seq).astype(BF16)
        for d in range(8):
            for g in range(8):
                o_mat[c, g * HALF:(g + 1) * HALF, d * LANES:(d + 1) * LANES] = (
                    res[d * HALF:(d + 1) * HALF, g * LANES:(g + 1) * LANES])

    def project_piece(c):
        return jnp.dot(o_mat[c], w_diag[c], preferred_element_type=F32)

    chip = me // 2

    def column_of(q, r, h):
        src = lax.rem(chip + r, n_dev // 2) * 2 + (core if q == 0 else 1 - core)
        return pl.multiple_of(src * (2 * HALF) + h * HALF, HALF)

    def out_copy(q, r, h):
        cols = pl.ds(column_of(q, r, h), HALF)
        return pltpu.make_async_copy(z_buf.at[:, cols, :], out_hbm.at[:, cols, :], out_sem.at[slot_of(q, r, h)])

    bias_out = bo_v[...].astype(F32).reshape(1, LANES)

    def finish(update, q, r, h):
        cols = pl.ds(column_of(q, r, h), HALF)
        for g in range(8):
            for k in range(4):
                i = g * 4 + k
                part = update[g * HALF:(g + 1) * HALF, k * LANES:(k + 1) * LANES] + bias_out
                z_buf[i, cols, :] = (z_buf[i, cols, :].astype(F32) + part).astype(BF16)
        out_copy(q, r, h).start()

    def half_unit(q, r, h):
        slot = slot_of(q, r, h)
        for c in range(PIECES):
            outer_piece(slot, c)
        update = project_piece(0)
        for c in range(1, PIECES):
            update = update + project_piece(c)
        finish(update, q, r, h)

    z_copy.wait()
    for h in range(2):
        half_unit(0, 0, h)
    for h in range(2):
        for c in range(PIECES):
            arrived(slot_of(1, 0, h), c)
        half_unit(1, 0, h)
    for h in range(2):
        for c in range(PIECES):
            arrived(slot_of(0, 3, h), c)
            if h == 0:
                send(to_right(3, h, c))
            send(to_sib(3, h, c))
            arrived(slot_of(0, 1, h), c)
            if h == 1:
                send(to_left(1, h, c))
            send(to_sib(1, h, c))
        half_unit(0, 3, h)
        half_unit(0, 1, h)
        for r in (3, 1):
            for c in range(PIECES):
                arrived(slot_of(1, r, h), c)
            half_unit(1, r, h)
    for c in range(PIECES):
        for h in range(2):
            arrived(slot_of(0, 2, h), c)
            send(to_sib(2, h, c))
        for q in range(2):
            for h in range(2):
                slot = slot_of(q, 2, h)
                if q == 1:
                    arrived(slot, c)
                outer_piece(slot, c)
                part = project_piece(c)
                if c < PIECES - 1:
                    u_acc[q, h] = part if c == 0 else u_acc[q, h] + part
                else:
                    finish(u_acc[q, h] + part, q, 2, h)
    for copy in sent:
        copy.wait_send()
    for q in range(2):
        for r in range(4):
            for h in range(2):
                out_copy(q, r, h).wait()


def solution(mesh):
    row_spec = P(('batch', 'dap'))
    col_spec = P(None, ('batch', 'dap'))
    rep_spec = P()
    n_dev = mesh.shape['dap']

    def local_update(z_rows, msa, ln_scale, ln_offset, w_a, b_a, w_b, b_b, w_out, b_out):
        n_seq, n_loc, m_dim = msa.shape
        hid = w_a.shape[1]
        pair = z_rows.shape[2]
        x = jnp.transpose(msa, (1, 2, 0)).reshape(n_loc * m_dim, n_seq)
        rows_piece = HALF * hid // PIECES
        any_spec = pl.BlockSpec(memory_space=pl.ANY)
        vmem = pltpu.VMEM
        dma = pltpu.SemaphoreType.DMA
        return pl.pallas_call(
            functools.partial(kernel, n_dev),
            out_shape=jax.ShapeDtypeStruct(z_rows.shape, BF16),
            in_specs=[any_spec] * 10,
            out_specs=any_spec,
            scratch_shapes=[
                vmem(z_rows.shape, BF16), vmem(x.shape, BF16),
                vmem((m_dim,), BF16), vmem((m_dim,), BF16),
                vmem((hid, m_dim), BF16), vmem((hid,), BF16), vmem((hid, m_dim), BF16), vmem((hid,), BF16),
                vmem(w_out.shape, BF16), vmem((pair,), BF16),
                vmem((m_dim, LANES), F32), vmem((m_dim, LANES), F32),
                vmem((4 * hid, LANES), F32), vmem((HALF * hid, LANES), F32), vmem((hid, LANES), F32),
                vmem((4 * hid, 4 * m_dim), BF16), vmem((HALF * hid, HALF * m_dim), BF16),
                vmem((n_seq, n_loc * hid), BF16),
                vmem((16, PIECES, rows_piece, n_seq), BF16),
                vmem((PIECES, LANES, 8 * LANES), BF16),
                vmem(w_out.shape, F32), vmem((PIECES, 8 * LANES, 4 * pair), BF16),
                vmem((2, 2, LANES, 4 * pair), F32),
                dma((8,)), dma((n_loc // 4,)), dma, dma((16,)), dma((16, PIECES)),
                dma((3, PIECES)), dma((3, PIECES)), dma((8, PIECES)),
            ],
            compiler_params=pltpu.CompilerParams(collective_id=0, has_side_effects=True, vmem_limit_bytes=60 * 1024 * 1024),
            name='outer_mean_ring',
        )(z_rows, x, ln_scale, ln_offset, w_a.T, b_a, w_b.T, b_b, w_out, b_out)

    return jax.shard_map(local_update, mesh=mesh, in_specs=(row_spec, col_spec) + (rep_spec,) * 8, out_specs=row_spec, check_vma=False)
```

```python
import functools

import jax
import jax.numpy as jnp
from jax import lax
from jax.experimental import pallas as pl
from jax.experimental.pallas import tpu as pltpu
from jax.sharding import PartitionSpec as P

LN_EPS = 1e-5
F32 = jnp.float32
BF16 = jnp.bfloat16
LANES = 128
HALF = 16
PIECES = 4
WHOLE = (0, 4)
OWN = ((0, 2), (2, 4))
FORWARD = ((0, 2), (2, 3), (3, 4))
LAST = 12
MESH = pl.DeviceIdType.MESH


def iota(shape, dim):
    return lax.broadcasted_iota(jnp.int32, shape, dim)


def column_lanes(row, count):
    spread = jnp.broadcast_to(row, (count, count))
    picked = jnp.where(iota((count, count), 0) == iota((count, count), 1), spread, 0.0)
    return jnp.broadcast_to(jnp.sum(picked, axis=1, keepdims=True), (count, LANES))


def kernel(n_dev, z_hbm, x_hbm, ls_hbm, lo_hbm, wa_hbm, ba_hbm, wb_hbm, bb_hbm, wo_hbm, bo_hbm,
           z_buf, a_mat, w_diag, u_last, bt_last,
           x_buf, ls_v, lo_v, wa_v, ba_v, wb_v, bb_v, wo_v, bo_v,
           scale_bc, offset_bc, bias_a, bias_b, row_bc, proj_a_w, proj_b_w, bt, o_mat, w_f32, u_acc,
           small_sem, x_sem, z_sem, recv_sem, send_sem):
    n_seq = x_hbm.shape[1]
    n_loc = z_hbm.shape[0]
    m_dim = wa_hbm.shape[1]
    hid = wa_hbm.shape[0]
    inv_seq = 1.0 / n_seq
    me = lax.axis_index('dap')
    core = lax.rem(me, 2)
    sib = me + 1 - 2 * core
    right = lax.rem(me + 2, n_dev)
    left = lax.rem(me + n_dev - 2, n_dev)

    barrier = pltpu.get_barrier_semaphore()
    for peer in (sib, right, left):
        pl.semaphore_signal(barrier, inc=1, device_id={'dap': peer}, device_id_type=MESH)

    small = [pltpu.make_async_copy(src, dst, small_sem.at[k]) for k, (src, dst) in enumerate((
        (wb_hbm, wb_v), (bb_hbm, bb_v), (ls_hbm, ls_v), (lo_hbm, lo_v), (wa_hbm, wa_v), (ba_hbm, ba_v),
        (wo_hbm, wo_v), (bo_hbm, bo_v)))]
    x_rows = 4 * m_dim
    x_copies = [pltpu.make_async_copy(x_hbm.at[pl.ds(k * x_rows, x_rows)], x_buf.at[pl.ds(k * x_rows, x_rows)], x_sem.at[k])
                for k in range(n_loc // 4)]
    for copy in small[:4]:
        copy.start()
    for copy in x_copies[:4]:
        copy.start()
    for copy in small[4:6]:
        copy.start()
    for copy in x_copies[4:]:
        copy.start()
    for copy in small[6:]:
        copy.start()
    z_copy = pltpu.make_async_copy(z_hbm, z_buf, z_sem)
    z_copy.start()

    for copy in small[:4]:
        copy.wait()
    row_bc[...] = column_lanes(bb_v[...].astype(F32).reshape(1, hid), hid)
    wb_rows = wb_v[...].astype(F32)
    wb_two = jnp.concatenate([wb_rows, wb_rows], axis=1)
    scale_bc[...] = column_lanes(ls_v[...].astype(F32).reshape(1, m_dim), m_dim)
    offset_bc[...] = column_lanes(lo_v[...].astype(F32).reshape(1, m_dim), m_dim)
    in_half = iota((HALF, LANES), 0)
    in_pair = iota((HALF, LANES), 1) // m_dim
    for d in range(hid):
        spread = jnp.broadcast_to(wb_two[d:d + 1, :], (HALF, LANES))
        for t in range(HALF * m_dim // LANES):
            part = jnp.where(in_half == in_pair + 2 * t, spread, 0.0)
            proj_b_w[d * HALF:(d + 1) * HALF, t * LANES:(t + 1) * LANES] = part.astype(BF16)
        bias_b[d * HALF:(d + 1) * HALF, :] = jnp.broadcast_to(row_bc[d:d + 1, :], (HALF, LANES))

    def norm_residue(n):
        rows = pl.ds(pl.multiple_of(n * m_dim, m_dim), m_dim)
        value = x_buf[rows, :].astype(F32)
        mean = jnp.sum(value, axis=0, keepdims=True) * (1.0 / m_dim)
        centred = value - mean
        var = jnp.sum(centred * centred, axis=0, keepdims=True) * (1.0 / m_dim)
        normed = centred * lax.rsqrt(var + LN_EPS)
        lanes4 = n_seq // LANES
        scale = jnp.concatenate([scale_bc[...]] * lanes4, axis=1)
        offset = jnp.concatenate([offset_bc[...]] * lanes4, axis=1)
        x_buf[rows, :] = (normed * scale + offset).astype(BF16)

    rows_piece = HALF * hid // PIECES

    def slot_of(q, r, h):
        return q * 8 + r * 2 + h

    def view(slot, group):
        if slot // 2 * 2 == LAST and group == FORWARD[-1]:
            return bt_last.at[slot % 2]
        return bt.at[slot, pl.ds(group[0], group[1] - group[0])]

    arrivals = {}

    def transfer(src, dst, group, peer):
        sem = recv_sem.at[arrivals.setdefault((dst, group), len(arrivals))]
        return pltpu.make_async_remote_copy(src_ref=view(src, group), dst_ref=view(dst, group), send_sem=send_sem,
                                            recv_sem=sem, device_id={'dap': peer}, device_id_type=MESH)

    def arrived(slot, group):
        transfer(slot, slot, group, sib).wait_recv()

    def send(src, dst, group, peer):
        transfer(src, dst, group, peer).start()

    for h in range(2):
        for k in range(4):
            x_copies[h * 4 + k].wait()

            def body(n, carry):
                norm_residue(n)
                return carry

            lax.fori_loop((h * 4 + k) * 4, (h * 4 + k + 1) * 4, body, 0, unroll=2)
        normed = x_buf.at[pl.ds(h * HALF * m_dim, HALF * m_dim), :]
        for c in range(PIECES):
            rows = slice(c * rows_piece, (c + 1) * rows_piece)
            res = jnp.dot(proj_b_w[rows, :], normed[...], preferred_element_type=F32)
            bias = jnp.concatenate([bias_b[rows, :]] * (n_seq // LANES), axis=1)
            bt[slot_of(0, 0, h), c] = (res + bias).astype(BF16)
        if h == 0:
            pl.semaphore_wait(barrier, 3)
        own = slot_of(0, 0, h)
        for group in OWN:
            send(own, slot_of(0, 3, h), group, right)
            send(own, slot_of(0, 1, h), group, left)
        send(own, slot_of(1, 0, h), WHOLE, sib)

    for copy in small[4:]:
        copy.wait()
    row_bc[...] = column_lanes(ba_v[...].astype(F32).reshape(1, hid), hid)
    bias_a[...] = jnp.concatenate([row_bc[...]] * 4, axis=0)
    wa_rows = wa_v[...].astype(F32)
    wa_wide = jnp.concatenate([jnp.concatenate([wa_rows] * 4, axis=1)] * 4, axis=0)
    same = (iota(wa_wide.shape, 0) // hid) == (iota(wa_wide.shape, 1) // m_dim)
    proj_a_w[...] = jnp.where(same, wa_wide, 0.0).astype(BF16)
    for g in range(n_loc // 4):
        res = jnp.dot(proj_a_w[...], x_buf[g * x_rows:(g + 1) * x_rows, :], preferred_element_type=F32)
        res = res + jnp.concatenate([bias_a[...]] * (n_seq // LANES), axis=1)
        a_mat[:, g * LANES:(g + 1) * LANES] = res.T.astype(BF16)

    w_f32[...] = wo_v[...].astype(F32)
    w_diag[...] = jnp.zeros_like(w_diag)

    def spread_w(d, carry):
        block = w_f32[pl.ds(d, hid, stride=hid), :].astype(BF16)
        c = d // 8
        for k in range(4):
            row = pl.multiple_of((d - c * 8) * LANES + k * hid, hid)
            w_diag[c, pl.ds(row, hid), k * LANES:(k + 1) * LANES] = block
        return carry

    lax.fori_loop(0, hid, spread_w, 0)

    def outer_piece(slot, c):
        res = jnp.dot(bt[slot, c], a_mat[...], preferred_element_type=F32)
        res = (res * inv_seq).astype(BF16)
        for d in range(8):
            for g in range(8):
                o_mat[c, g * HALF:(g + 1) * HALF, d * LANES:(d + 1) * LANES] = (
                    res[d * HALF:(d + 1) * HALF, g * LANES:(g + 1) * LANES])

    def project_piece(c):
        return jnp.dot(o_mat[c], w_diag[c], preferred_element_type=F32)

    chip = me // 2

    def column_of(q, r, h):
        src = lax.rem(chip + r, n_dev // 2) * 2 + (core if q == 0 else 1 - core)
        return pl.multiple_of(src * (2 * HALF) + h * HALF, HALF)

    bias_out = bo_v[...].astype(F32).reshape(1, LANES)

    def finish(update, q, r, h):
        cols = pl.ds(column_of(q, r, h), HALF)
        for g in range(8):
            for k in range(4):
                i = g * 4 + k
                part = update[g * HALF:(g + 1) * HALF, k * LANES:(k + 1) * LANES] + bias_out
                z_buf[i, cols, :] = (z_buf[i, cols, :].astype(F32) + part).astype(BF16)

    def half_unit(q, r, h):
        slot = slot_of(q, r, h)
        for c in range(PIECES):
            outer_piece(slot, c)
        update = project_piece(0)
        for c in range(1, PIECES):
            update = update + project_piece(c)
        finish(update, q, r, h)

    z_copy.wait()
    for h in range(2):
        half_unit(0, 0, h)
    for h in range(2):
        arrived(slot_of(1, 0, h), WHOLE)
        half_unit(1, 0, h)
    for h in range(2):
        for group in OWN:
            arrived(slot_of(0, 3, h), group)
            arrived(slot_of(0, 1, h), group)
            for piece in FORWARD:
                if group[0] <= piece[0] < group[1]:
                    if h == 0:
                        send(slot_of(0, 3, 0), slot_of(0, 2, 0), piece, right)
                    else:
                        send(slot_of(0, 1, 1), slot_of(0, 2, 1), piece, left)
        for r in (3, 1):
            send(slot_of(0, r, h), slot_of(1, r, h), WHOLE, sib)
        for r in (3, 1):
            half_unit(0, r, h)
        for r in (3, 1):
            arrived(slot_of(1, r, h), WHOLE)
            half_unit(1, r, h)

    def part_unit(q, h, group):
        for c in range(*group):
            outer_piece(slot_of(q, 2, h), c)
        update = project_piece(group[0])
        for c in range(group[0] + 1, group[1]):
            update = update + project_piece(c)
        return update

    for group in FORWARD:
        first, last = group == FORWARD[0], group == FORWARD[-1]
        for h in range(2):
            arrived(slot_of(0, 2, h), group)
            send(slot_of(0, 2, h), slot_of(1, 2, h), group, sib)
        for h in range(2):
            update = part_unit(0, h, group)
            if last:
                finish(u_acc[h] + update, 0, 2, h)
            else:
                u_acc[h] = update if first else u_acc[h] + update
        for h in range(2):
            arrived(slot_of(1, 2, h), group)
            if not last:
                update = part_unit(1, h, group)
                if first:
                    update = update + jnp.concatenate([bias_out] * 4, axis=1)
                u_last[h] = update if first else u_last[h] + update
    pltpu.make_async_remote_copy(src_ref=bt.at[pl.ds(0, 14)], dst_ref=bt.at[pl.ds(0, 14)], send_sem=send_sem,
                                 recv_sem=recv_sem.at[0], device_id={'dap': sib}, device_id_type=MESH).wait_send()


def last_kernel(n_dev, z_buf, a_mat, w_diag, u_last, bt_last, out_hbm, cols_buf, sem):
    width = 2 * HALF
    inv_seq = 1.0 / a_mat.shape[0]
    me = lax.axis_index('dap')
    chips = n_dev // 2
    mine = lax.rem(me // 2 + 2, chips) * 2 + 1 - lax.rem(me, 2)

    def block(k):
        return pl.ds(pl.multiple_of(lax.rem(mine + k, n_dev) * width, width), width)

    copies = [pltpu.make_async_copy(z_buf.at[:, block(k), :], out_hbm.at[:, block(k), :], sem.at[k]) for k in range(1, n_dev)]
    for copy in copies:
        copy.start()
    c = PIECES - 1
    for h in range(2):
        res = jnp.dot(bt_last[h, 0], a_mat[...], preferred_element_type=F32)
        res = (res * inv_seq).astype(BF16)
        wide = jnp.concatenate(
            [jnp.concatenate([res[d * HALF:(d + 1) * HALF, g * LANES:(g + 1) * LANES] for d in range(8)], axis=1)
             for g in range(8)], axis=0)
        update = u_last[h] + jnp.dot(wide, w_diag[c], preferred_element_type=F32)
        cols = pl.ds(pl.multiple_of(mine * width + h * HALF, HALF), HALF)
        for g in range(8):
            for k in range(4):
                i = g * 4 + k
                part = update[g * HALF:(g + 1) * HALF, k * LANES:(k + 1) * LANES]
                cols_buf[i, h * HALF:(h + 1) * HALF, :] = (z_buf[i, cols, :].astype(F32) + part).astype(BF16)
    copy = pltpu.make_async_copy(cols_buf, out_hbm.at[:, block(0), :], sem.at[0])
    copy.start()
    copies.append(copy)
    for copy in copies:
        copy.wait()


def solution(mesh):
    row_spec = P(('batch', 'dap'))
    col_spec = P(None, ('batch', 'dap'))
    rep_spec = P()
    n_dev = mesh.shape['dap']

    def local_update(z_rows, msa, ln_scale, ln_offset, w_a, b_a, w_b, b_b, w_out, b_out):
        n_seq, n_loc, m_dim = msa.shape
        hid = w_a.shape[1]
        pair = z_rows.shape[2]
        x = jnp.transpose(msa, (1, 2, 0)).reshape(n_loc * m_dim, n_seq)
        rows_piece = HALF * hid // PIECES
        any_spec = pl.BlockSpec(memory_space=pl.ANY)
        vmem = pltpu.VMEM
        dma = pltpu.SemaphoreType.DMA
        outs = [
            vmem(z_rows.shape, BF16), vmem((n_seq, n_loc * hid), BF16), vmem((PIECES, 8 * LANES, 4 * pair), BF16),
            vmem((2, LANES, 4 * pair), F32), vmem((2, 1, rows_piece, n_seq), BF16),
        ]
        vmem_spec = pl.BlockSpec(memory_space=pltpu.VMEM)
        made = pl.pallas_call(
            functools.partial(kernel, n_dev),
            out_shape=outs,
            in_specs=[any_spec] * 10,
            out_specs=[vmem_spec] * len(outs),
            scratch_shapes=[
                vmem(x.shape, BF16),
                vmem((m_dim,), BF16), vmem((m_dim,), BF16),
                vmem((hid, m_dim), BF16), vmem((hid,), BF16), vmem((hid, m_dim), BF16), vmem((hid,), BF16),
                vmem(w_out.shape, BF16), vmem((pair,), BF16),
                vmem((m_dim, LANES), F32), vmem((m_dim, LANES), F32),
                vmem((4 * hid, LANES), F32), vmem((HALF * hid, LANES), F32), vmem((hid, LANES), F32),
                vmem((4 * hid, 4 * m_dim), BF16), vmem((HALF * hid, HALF * m_dim), BF16),
                vmem((16, PIECES, rows_piece, n_seq), BF16),
                vmem((PIECES, LANES, 8 * LANES), BF16),
                vmem(w_out.shape, F32),
                vmem((2, LANES, 4 * pair), F32),
                dma((8,)), dma((n_loc // 4,)), dma, dma((26,)), dma,
            ],
            compiler_params=pltpu.CompilerParams(collective_id=0, has_side_effects=True, vmem_limit_bytes=44 * 1024 * 1024),
            name='outer_mean_ring',
        )(z_rows, x, ln_scale, ln_offset, w_a.T, b_a, w_b.T, b_b, w_out, b_out)
        made = [pltpu.with_memory_space_constraint(part, pltpu.VMEM) for part in made]
        return pl.pallas_call(
            functools.partial(last_kernel, n_dev),
            out_shape=jax.ShapeDtypeStruct(z_rows.shape, BF16),
            in_specs=[vmem_spec] * len(outs),
            out_specs=any_spec,
            scratch_shapes=[vmem((n_loc, 2 * HALF, pair), BF16), dma((n_dev,))],
            compiler_params=pltpu.CompilerParams(vmem_limit_bytes=8 * 1024 * 1024),
            name='outer_mean_last',
        )(*made)

    return jax.shard_map(local_update, mesh=mesh, in_specs=(row_spec, col_spec) + (rep_spec,) * 8, out_specs=row_spec, check_vma=False)
```

```python
import functools

import jax
import jax.numpy as jnp
from jax import lax
from jax.experimental import pallas as pl
from jax.experimental.pallas import tpu as pltpu
from jax.sharding import PartitionSpec as P

LN_EPS = 1e-5
F32 = jnp.float32
BF16 = jnp.bfloat16
LANES = 128
HALF = 16
PIECES = 4
BLOCK = 128
ALL = ('rows', 0, 4)
FIRST_OWN = (('lanes', 0), ('lanes', 1))
SECOND_OWN = (('rows', 0, 2), ('rows', 2, 4))
SHARED = (('rows', 0, 2), ('rows', 2, 3))
FINAL = ('rows', 3, 4)
MESH = pl.DeviceIdType.MESH


def iota(shape, dim):
    return lax.broadcasted_iota(jnp.int32, shape, dim)


def column_lanes(row, count):
    spread = jnp.broadcast_to(row, (count, count))
    picked = jnp.where(iota((count, count), 0) == iota((count, count), 1), spread, 0.0)
    return jnp.broadcast_to(jnp.sum(picked, axis=1, keepdims=True), (count, LANES))


def kernel(n_dev, z_hbm, x_hbm, ls_hbm, lo_hbm, wa_hbm, ba_hbm, wb_hbm, bb_hbm, wo_hbm, bo_hbm,
           z_buf, a_mat, w_last, u_last, bt_last,
           x_buf, ls_v, lo_v, wa_v, ba_v, wb_v, bb_v, wo_v, bo_v,
           scale_bc, offset_bc, bias_a, bias_b, row_bc, proj_a_w, proj_b_w, bt, o_mat, w_f32, w_diag,
           small_sem, x_sem, z_sem, recv_sem, send_sem):
    n_seq = x_hbm.shape[1]
    n_loc = z_hbm.shape[0]
    m_dim = wa_hbm.shape[1]
    hid = wa_hbm.shape[0]
    inv_seq = 1.0 / n_seq
    me = lax.axis_index('dap')
    core = lax.rem(me, 2)
    sib = me + 1 - 2 * core
    right = lax.rem(me + 2, n_dev)
    left = lax.rem(me + n_dev - 2, n_dev)

    barrier = pltpu.get_barrier_semaphore()
    for peer in (sib, right, left):
        pl.semaphore_signal(barrier, inc=1, device_id={'dap': peer}, device_id_type=MESH)

    small = [pltpu.make_async_copy(src, dst, small_sem.at[k]) for k, (src, dst) in enumerate((
        (wb_hbm, wb_v), (bb_hbm, bb_v), (ls_hbm, ls_v), (lo_hbm, lo_v), (wa_hbm, wa_v), (ba_hbm, ba_v),
        (wo_hbm, wo_v), (bo_hbm, bo_v)))]
    half_rows = HALF * m_dim
    half_seq = n_seq // 2
    parts = [(slice(k * half_rows // 2, (k + 1) * half_rows // 2), slice(p * half_seq, (p + 1) * half_seq))
             for p in range(2) for k in range(2)]
    parts += [(slice(half_rows + k * half_rows // 2, half_rows + (k + 1) * half_rows // 2), slice(0, n_seq)) for k in range(2)]
    x_copies = [pltpu.make_async_copy(x_hbm.at[part], x_buf.at[part], x_sem.at[k]) for k, part in enumerate(parts)]
    for copy in x_copies[:2] + small[:4] + x_copies[2:4]:
        copy.start()
    z_copy = pltpu.make_async_copy(z_hbm, z_buf, z_sem)

    for copy in small[:4]:
        copy.wait()
    row_bc[...] = column_lanes(bb_v[...].astype(F32).reshape(1, hid), hid)
    wb_rows = wb_v[...].astype(F32)
    wb_two = jnp.concatenate([wb_rows, wb_rows], axis=1)
    scale_bc[...] = column_lanes(ls_v[...].astype(F32).reshape(1, m_dim), m_dim)
    offset_bc[...] = column_lanes(lo_v[...].astype(F32).reshape(1, m_dim), m_dim)
    in_half = iota((HALF, LANES), 0)
    in_pair = iota((HALF, LANES), 1) // m_dim
    for d in range(hid):
        spread = jnp.broadcast_to(wb_two[d:d + 1, :], (HALF, LANES))
        for t in range(HALF * m_dim // LANES):
            part = jnp.where(in_half == in_pair + 2 * t, spread, 0.0)
            proj_b_w[d * HALF:(d + 1) * HALF, t * LANES:(t + 1) * LANES] = part.astype(BF16)
        bias_b[d * HALF:(d + 1) * HALF, :] = jnp.broadcast_to(row_bc[d:d + 1, :], (HALF, LANES))

    def norm_part(rows, lanes):
        width = lanes.stop - lanes.start
        scale = jnp.concatenate([scale_bc[...]] * (width // LANES), axis=1)
        offset = jnp.concatenate([offset_bc[...]] * (width // LANES), axis=1)

        def body(n, carry):
            at = (pl.ds(pl.multiple_of(rows.start + n * m_dim, m_dim), m_dim), lanes)
            value = x_buf[at].astype(F32)
            mean = jnp.sum(value, axis=0, keepdims=True) * (1.0 / m_dim)
            centred = value - mean
            var = jnp.sum(centred * centred, axis=0, keepdims=True) * (1.0 / m_dim)
            normed = centred * lax.rsqrt(var + LN_EPS)
            x_buf[at] = (normed * scale + offset).astype(BF16)
            return carry

        lax.fori_loop(0, (rows.stop - rows.start) // m_dim, body, 0, unroll=4)

    def slot_of(q, r, h):
        return q * 8 + r * 2 + h

    def view(q, r, h, group):
        slot = slot_of(q, r, h)
        if group[0] == 'lanes':
            return bt.at[slot, group[1]]
        if r == 2 and group == FINAL and q == 1:
            return bt_last.at[h]
        if group == ALL:
            return bt.at[slot]
        return bt.at[slot, :, pl.ds(group[1] * BLOCK, (group[2] - group[1]) * BLOCK), :]

    sems = {}

    def transfer(q, r, h, group, peer, r_there):
        if r_there == 2:
            k = SHARED.index(group) if group != FINAL else 2
        else:
            k = 0 if group in (ALL, FIRST_OWN[0], SECOND_OWN[0]) else 1
        k = sems.setdefault((r_there, h, k), len(sems))
        return pltpu.make_async_remote_copy(
            src_ref=view(q, r, h, group), dst_ref=view(q, r_there, h, group), send_sem=send_sem,
            recv_sem=recv_sem.at[q * 16 + k], device_id={'dap': peer}, device_id_type=MESH)

    def arrived(q, r, h, group):
        transfer(q, r, h, group, sib, r).wait_recv()

    def to_right(q, r, h, group):
        transfer(q, r, h, group, right, (r + 3) % 4).start()

    def to_left(q, r, h, group):
        transfer(q, r, h, group, left, (r + 1) % 4).start()

    def to_sib(q, r, h, group):
        transfer(q, r, h, group, sib, r).start()

    own, other = core, 1 - core

    def project_b(h, c, lanes):
        rows = slice(c * BLOCK, (c + 1) * BLOCK)
        width = lanes.stop - lanes.start
        res = jnp.dot(proj_b_w[rows, :], x_buf[h * half_rows:(h + 1) * half_rows, lanes], preferred_element_type=F32)
        res = (res + jnp.concatenate([bias_b[rows, :]] * (width // LANES), axis=1)).astype(BF16)
        for k in range(width // half_seq):
            bt[slot_of(own, 0, h), lanes.start // half_seq + k, rows, :] = res[:, k * half_seq:(k + 1) * half_seq]

    for p in range(2):
        for k in range(2):
            x_copies[2 * p + k].wait()
            norm_part(*parts[2 * p + k])
        if p == 0:
            for copy in x_copies[4:] + small[4:] + [z_copy]:
                copy.start()
        for c in range(PIECES):
            project_b(0, c, parts[2 * p][1])
        if p == 0:
            pl.semaphore_wait(barrier, 3)
        to_right(own, 0, 0, FIRST_OWN[p])
        to_left(own, 0, 0, FIRST_OWN[p])
    to_sib(own, 0, 0, ALL)
    for k in range(2):
        x_copies[4 + k].wait()
        norm_part(*parts[4 + k])
    for group in SECOND_OWN:
        for c in range(*group[1:]):
            project_b(1, c, parts[4][1])
        to_right(own, 0, 1, group)
        to_left(own, 0, 1, group)
    to_sib(own, 0, 1, ALL)

    for copy in small[4:]:
        copy.wait()
    row_bc[...] = column_lanes(ba_v[...].astype(F32).reshape(1, hid), hid)
    bias_a[...] = jnp.concatenate([row_bc[...]] * 4, axis=0)
    wa_rows = wa_v[...].astype(F32)
    wa_wide = jnp.concatenate([jnp.concatenate([wa_rows] * 4, axis=1)] * 4, axis=0)
    same = (iota(wa_wide.shape, 0) // hid) == (iota(wa_wide.shape, 1) // m_dim)
    proj_a_w[...] = jnp.where(same, wa_wide, 0.0).astype(BF16)
    for g in range(n_loc // 4):
        res = jnp.dot(proj_a_w[...], x_buf[g * 4 * m_dim:(g + 1) * 4 * m_dim, :], preferred_element_type=F32)
        res = res + jnp.concatenate([bias_a[...]] * (n_seq // LANES), axis=1)
        a_mat[:, g * LANES:(g + 1) * LANES] = res.T.astype(BF16)

    w_f32[...] = wo_v[...].astype(F32)
    w_diag[...] = jnp.zeros_like(w_diag)
    w_last[...] = jnp.zeros_like(w_last)

    def spread_w(d, at):
        block = w_f32[pl.ds(d, hid, stride=hid), :].astype(BF16)
        for k in range(4):
            row = pl.multiple_of(lax.rem(d, 8) * LANES + k * hid, hid)
            at[pl.ds(row, hid), k * LANES:(k + 1) * LANES] = block

    for c in range(PIECES):
        at = w_diag.at[c] if c < PIECES - 1 else w_last

        def body(d, carry):
            spread_w(d, at)
            return carry

        lax.fori_loop(c * 8, (c + 1) * 8, body, 0)

    def outer_piece(slot, c):
        rows = slice(c * BLOCK, (c + 1) * BLOCK)
        lhs = jnp.concatenate([bt[slot, 0, rows, :], bt[slot, 1, rows, :]], axis=1)
        res = jnp.dot(lhs, a_mat[...], preferred_element_type=F32)
        res = (res * inv_seq).astype(BF16)
        for d in range(8):
            for g in range(8):
                o_mat[c, g * HALF:(g + 1) * HALF, d * LANES:(d + 1) * LANES] = (
                    res[d * HALF:(d + 1) * HALF, g * LANES:(g + 1) * LANES])

    def project_piece(c):
        return jnp.dot(o_mat[c], w_diag[c] if c < PIECES - 1 else w_last[...], preferred_element_type=F32)

    chip = me // 2

    def column_of(q, r, h):
        src = lax.rem(chip + r, n_dev // 2) * 2 + q
        return pl.multiple_of(src * (2 * HALF) + h * HALF, HALF)

    bias_out = bo_v[...].astype(F32).reshape(1, LANES)

    def finish(update, bias, q, r, h):
        cols = pl.ds(column_of(q, r, h), HALF)
        for g in range(8):
            for k in range(4):
                i = g * 4 + k
                part = update[g * HALF:(g + 1) * HALF, k * LANES:(k + 1) * LANES]
                if bias is not None:
                    part = part + bias
                z_buf[i, cols, :] = (z_buf[i, cols, :].astype(F32) + part).astype(BF16)

    def half_unit(q, r, h):
        slot = slot_of(q, r, h)
        for c in range(PIECES):
            outer_piece(slot, c)
        update = project_piece(0)
        for c in range(1, PIECES):
            update = update + project_piece(c)
        finish(update, bias_out, q, r, h)

    z_copy.wait()
    for h in range(2):
        half_unit(own, 0, h)
    for h in range(2):
        arrived(other, 0, h, ALL)
        half_unit(other, 0, h)
    for h in range(2):
        for k, group in enumerate(FIRST_OWN if h == 0 else SECOND_OWN):
            arrived(own, 3, h, group)
            arrived(own, 1, h, group)
            if h == 1:
                to_left(own, 1, 1, SHARED[k])
        if h == 0:
            for group in SHARED:
                to_right(own, 3, 0, group)
        for r in (3, 1):
            to_sib(own, r, h, ALL)
        for r in (3, 1):
            half_unit(own, r, h)
        for r in (3, 1):
            arrived(other, r, h, ALL)

        @pl.when(core == 1)
        def _():
            for q in range(2):
                if h == 0:
                    to_right(q, 3, 0, FINAL)
                else:
                    to_left(q, 1, 1, FINAL)

        for r in (3, 1):
            half_unit(other, r, h)

    def part_unit(q, h, group):
        slot = slot_of(q, 2, h)
        for c in range(*group[1:]):
            outer_piece(slot, c)
        update = project_piece(group[1])
        for c in range(group[1] + 1, group[2]):
            update = update + project_piece(c)
        return update

    wide_bias = jnp.concatenate([bias_out] * 4, axis=1)
    for group in SHARED:
        for h in range(2):
            arrived(own, 2, h, group)
            to_sib(own, 2, h, group)
        for q in (own, other):
            for h in range(2):
                if q is other:
                    arrived(other, 2, h, group)
                update = part_unit(q, h, group)
                u_last[q, h] = update + wide_bias if group is SHARED[0] else u_last[q, h] + update
    for h in range(2):
        arrived(0, 2, h, FINAL)

        @pl.when(core == 1)
        def _():
            to_sib(0, 2, h, FINAL)

    for h in range(2):
        finish(u_last[0, h] + part_unit(0, h, FINAL), None, 0, 2, h)
    for h in range(2):
        arrived(1, 2, h, FINAL)

        @pl.when(core == 1)
        def _():
            to_sib(1, 2, h, FINAL)

    for q, slots in enumerate((13, 15)):
        @pl.when(core == q)
        def _():
            everything = bt.at[pl.ds(0, slots)]
            pltpu.make_async_remote_copy(src_ref=everything, dst_ref=everything, send_sem=send_sem, recv_sem=recv_sem.at[0],
                                         device_id={'dap': sib}, device_id_type=MESH).wait_send()


def last_kernel(n_dev, z_buf, a_mat, w_last, u_last, bt_last, out_hbm, cols_buf, sem):
    width = 2 * HALF
    inv_seq = 1.0 / a_mat.shape[0]
    me = lax.axis_index('dap')
    chips = n_dev // 2
    mine = lax.rem(me // 2 + 2, chips) * 2 + 1

    def block(k):
        return pl.ds(pl.multiple_of(lax.rem(mine + k, n_dev) * width, width), width)

    copies = [pltpu.make_async_copy(z_buf.at[:, block(k), :], out_hbm.at[:, block(k), :], sem.at[k]) for k in range(1, n_dev)]
    for copy in copies:
        copy.start()
    lhs = jnp.concatenate([jnp.concatenate([bt_last[h, 0], bt_last[h, 1]], axis=1) for h in range(2)], axis=0)
    res = jnp.dot(lhs, a_mat[...], preferred_element_type=F32)
    res = (res * inv_seq).astype(BF16)
    wide = jnp.concatenate(
        [jnp.concatenate([res[h * BLOCK + d * HALF:h * BLOCK + (d + 1) * HALF, g * LANES:(g + 1) * LANES] for d in range(8)], axis=1)
         for h in range(2) for g in range(8)], axis=0)
    update = jnp.dot(wide, w_last[...], preferred_element_type=F32)
    for h in range(2):
        cols = pl.ds(pl.multiple_of(mine * width + h * HALF, HALF), HALF)
        for g in range(8):
            for k in range(4):
                i = g * 4 + k
                rows, lanes = slice(g * HALF, (g + 1) * HALF), slice(k * LANES, (k + 1) * LANES)
                part = u_last[1, h, rows, lanes] + update[h * BLOCK + g * HALF:h * BLOCK + (g + 1) * HALF, lanes]
                cols_buf[i, h * HALF:(h + 1) * HALF, :] = (z_buf[i, cols, :].astype(F32) + part).astype(BF16)
    copy = pltpu.make_async_copy(cols_buf, out_hbm.at[:, block(0), :], sem.at[0])
    copy.start()
    copies.append(copy)
    for copy in copies:
        copy.wait()


def solution(mesh):
    row_spec = P(('batch', 'dap'))
    col_spec = P(None, ('batch', 'dap'))
    rep_spec = P()
    n_dev = mesh.shape['dap']

    def local_update(z_rows, msa, ln_scale, ln_offset, w_a, b_a, w_b, b_b, w_out, b_out):
        n_seq, n_loc, m_dim = msa.shape
        hid = w_a.shape[1]
        pair = z_rows.shape[2]
        x = jnp.transpose(msa, (1, 2, 0)).reshape(n_loc * m_dim, n_seq)
        any_spec = pl.BlockSpec(memory_space=pltpu.HBM)
        vmem = pltpu.VMEM
        dma = pltpu.SemaphoreType.DMA
        outs = [
            vmem(z_rows.shape, BF16), vmem((n_seq, n_loc * hid), BF16), vmem((8 * LANES, 4 * pair), BF16),
            vmem((2, 2, LANES, 4 * pair), F32), vmem((2, 2, BLOCK, n_seq // 2), BF16),
        ]
        vmem_spec = pl.BlockSpec(memory_space=pltpu.VMEM)
        made = pl.pallas_call(
            functools.partial(kernel, n_dev),
            out_shape=outs,
            in_specs=[any_spec] * 10,
            out_specs=[vmem_spec] * len(outs),
            scratch_shapes=[
                vmem(x.shape, BF16),
                vmem((m_dim,), BF16), vmem((m_dim,), BF16),
                vmem((hid, m_dim), BF16), vmem((hid,), BF16), vmem((hid, m_dim), BF16), vmem((hid,), BF16),
                vmem(w_out.shape, BF16), vmem((pair,), BF16),
                vmem((m_dim, LANES), F32), vmem((m_dim, LANES), F32),
                vmem((4 * hid, LANES), F32), vmem((HALF * hid, LANES), F32), vmem((hid, LANES), F32),
                vmem((4 * hid, 4 * m_dim), BF16), vmem((HALF * hid, HALF * m_dim), BF16),
                vmem((16, 2, PIECES * BLOCK, n_seq // 2), BF16),
                vmem((PIECES, LANES, 8 * LANES), BF16),
                vmem(w_out.shape, F32), vmem((PIECES - 1, 8 * LANES, 4 * pair), BF16),
                dma((8,)), dma((6,)), dma, dma((32,)), dma,
            ],
            compiler_params=pltpu.CompilerParams(collective_id=0, has_side_effects=True, vmem_limit_bytes=54 * 1024 * 1024),
            name='outer_mean_ring',
        )(*[pltpu.with_memory_space_constraint(part, pltpu.HBM)
            for part in (z_rows, x, ln_scale, ln_offset, w_a.T, b_a, w_b.T, b_b, w_out, b_out)])
        made = [pltpu.with_memory_space_constraint(part, pltpu.VMEM) for part in made]
        return pl.pallas_call(
            functools.partial(last_kernel, n_dev),
            out_shape=jax.ShapeDtypeStruct(z_rows.shape, BF16),
            in_specs=[vmem_spec] * len(outs),
            out_specs=any_spec,
            scratch_shapes=[vmem((n_loc, 2 * HALF, pair), BF16), dma((n_dev,))],
            compiler_params=pltpu.CompilerParams(vmem_limit_bytes=8 * 1024 * 1024),
            name='outer_mean_last',
        )(*made)

    return jax.shard_map(local_update, mesh=mesh, in_specs=(row_spec, col_spec) + (rep_spec,) * 8, out_specs=row_spec, check_vma=False)
```

```python
import functools

import jax
import jax.numpy as jnp
from jax import lax
from jax.experimental import pallas as pl
from jax.experimental.pallas import tpu as pltpu
from jax.sharding import PartitionSpec as P

LN_EPS = 1e-5
F32 = jnp.float32
BF16 = jnp.bfloat16
LANES = 128
HALF = 16
PIECES = 4
BLOCK = 128
ALL = ('rows', 0, 4)
FIRST_OWN = (('lanes', 0, 128), ('lanes', 128, 256), ('lanes', 256, 512))
SECOND_OWN = (('rows', 0, 2), ('rows', 2, 4))
SHARED = (('rows', 0, 2), ('rows', 2, 3))
FINAL = ('rows', 3, 4)
MESH = pl.DeviceIdType.MESH


def iota(shape, dim):
    return lax.broadcasted_iota(jnp.int32, shape, dim)


def column_lanes(row, count):
    spread = jnp.broadcast_to(row, (count, count))
    picked = jnp.where(iota((count, count), 0) == iota((count, count), 1), spread, 0.0)
    return jnp.broadcast_to(jnp.sum(picked, axis=1, keepdims=True), (count, LANES))


def pair_product(lhs, a_mat, w_part, inv_seq):
    res = jnp.dot(jnp.concatenate(lhs, axis=0), a_mat[...], preferred_element_type=F32)
    res = (res * inv_seq).astype(BF16)
    wide = jnp.concatenate(
        [jnp.concatenate([res[h * BLOCK + d * HALF:h * BLOCK + (d + 1) * HALF, g * LANES:(g + 1) * LANES] for d in range(8)], axis=1)
         for h in range(2) for g in range(8)], axis=0)
    return jnp.dot(wide, w_part, preferred_element_type=F32)


def kernel(n_dev, z_hbm, x_hbm, ls_hbm, lo_hbm, wa_hbm, ba_hbm, wb_hbm, bb_hbm, wo_hbm, bo_hbm,
           z_buf, a_mat, w_last, u_last, bt_last,
           x_buf, ls_v, lo_v, wa_v, ba_v, wb_v, bb_v, wo_v, bo_v,
           scale_bc, offset_bc, bias_a, bias_b, row_bc, proj_a_w, proj_b_w, bt, o_mat, w_f32, w_diag,
           small_sem, x_sem, z_sem, recv_sem, send_sem):
    n_seq = x_hbm.shape[1]
    n_loc = z_hbm.shape[0]
    m_dim = wa_hbm.shape[1]
    hid = wa_hbm.shape[0]
    inv_seq = 1.0 / n_seq
    me = lax.axis_index('dap')
    core = lax.rem(me, 2)
    sib = me + 1 - 2 * core
    right = lax.rem(me + 2, n_dev)
    left = lax.rem(me + n_dev - 2, n_dev)

    barrier = pltpu.get_barrier_semaphore()
    for peer in (sib, right, left):
        pl.semaphore_signal(barrier, inc=1, device_id={'dap': peer}, device_id_type=MESH)

    small = [pltpu.make_async_copy(src, dst, small_sem.at[k]) for k, (src, dst) in enumerate((
        (wb_hbm, wb_v), (bb_hbm, bb_v), (ls_hbm, ls_v), (lo_hbm, lo_v), (wa_hbm, wa_v), (ba_hbm, ba_v),
        (wo_hbm, wo_v), (bo_hbm, bo_v)))]
    half_rows = HALF * m_dim
    half_seq = n_seq // 2
    parts = [(slice(k * half_rows // 2, (k + 1) * half_rows // 2), slice(*group[1:]))
             for group in FIRST_OWN for k in range(2)]
    parts += [(slice(half_rows + k * half_rows // 2, half_rows + (k + 1) * half_rows // 2), slice(0, n_seq)) for k in range(2)]
    x_copies = [pltpu.make_async_copy(x_hbm.at[part], x_buf.at[part], x_sem.at[k]) for k, part in enumerate(parts)]
    for copy in small[:4] + x_copies[:6]:
        copy.start()
    z_copy = pltpu.make_async_copy(z_hbm, z_buf, z_sem)

    for copy in small[:4]:
        copy.wait()
    row_bc[...] = column_lanes(bb_v[...].astype(F32).reshape(1, hid), hid)
    wb_rows = wb_v[...].astype(F32)
    wb_two = jnp.concatenate([wb_rows, wb_rows], axis=1)
    scale_bc[...] = column_lanes(ls_v[...].astype(F32).reshape(1, m_dim), m_dim)
    offset_bc[...] = column_lanes(lo_v[...].astype(F32).reshape(1, m_dim), m_dim)
    in_eight = iota((8, LANES), 0)
    in_pair = iota((8, LANES), 1) // m_dim
    for d in range(0, hid, 2):
        for t in range(8 * m_dim // LANES):
            part = [jnp.where(in_eight == in_pair + 2 * t, jnp.broadcast_to(wb_two[e:e + 1, :], (8, LANES)), 0.0)
                    for e in (d, d + 1)]
            proj_b_w[d * 8:(d + 2) * 8, t * LANES:(t + 1) * LANES] = jnp.concatenate(part, axis=0).astype(BF16)
        for e in (d, d + 1):
            bias_b[e * 8:(e + 1) * 8, :] = jnp.broadcast_to(row_bc[e:e + 1, :], (8, LANES))

    def norm_part(rows, lanes):
        width = lanes.stop - lanes.start
        scale = jnp.concatenate([scale_bc[...]] * (width // LANES), axis=1)
        offset = jnp.concatenate([offset_bc[...]] * (width // LANES), axis=1)

        def body(n, carry):
            at = (pl.ds(pl.multiple_of(rows.start + n * m_dim, m_dim), m_dim), lanes)
            value = x_buf[at].astype(F32)
            mean = jnp.sum(value, axis=0, keepdims=True) * (1.0 / m_dim)
            centred = value - mean
            var = jnp.sum(centred * centred, axis=0, keepdims=True) * (1.0 / m_dim)
            normed = centred * lax.rsqrt(var + LN_EPS)
            x_buf[at] = (normed * scale + offset).astype(BF16)
            return carry

        lax.fori_loop(0, (rows.stop - rows.start) // m_dim, body, 0, unroll=8)

    def slot_of(q, r, h):
        return q * 8 + r * 2 + h

    def view(q, r, h, group):
        slot = slot_of(q, r, h)
        if group[0] == 'lanes':
            k = group[1] // half_seq
            return bt.at[slot, k, :, pl.ds(group[1] - k * half_seq, group[2] - group[1])]
        if r == 2 and group == FINAL and q == 1:
            return bt_last.at[h]
        if group == ALL:
            return bt.at[slot]
        return bt.at[slot, :, pl.ds(group[1] * BLOCK, (group[2] - group[1]) * BLOCK), :]

    sems = {}

    def transfer(q, r, h, group, peer, r_there):
        if r_there == 2:
            k = SHARED.index(group) if group != FINAL else 2
        else:
            k = 0 if group == ALL else (FIRST_OWN if group in FIRST_OWN else SECOND_OWN).index(group)
        k = sems.setdefault((r_there, h, k), len(sems))
        return pltpu.make_async_remote_copy(
            src_ref=view(q, r, h, group), dst_ref=view(q, r_there, h, group), send_sem=send_sem,
            recv_sem=recv_sem.at[q * 18 + k], device_id={'dap': peer}, device_id_type=MESH)

    def arrived(q, r, h, group):
        transfer(q, r, h, group, sib, r).wait_recv()

    def to_right(q, r, h, group):
        transfer(q, r, h, group, right, (r + 3) % 4).start()

    def to_left(q, r, h, group):
        transfer(q, r, h, group, left, (r + 1) % 4).start()

    def to_sib(q, r, h, group):
        transfer(q, r, h, group, sib, r).start()

    own, other = core, 1 - core

    def project_b(h, lanes):
        width = lanes.stop - lanes.start
        bias = jnp.concatenate([bias_b[...]] * (width // LANES), axis=1)
        res = [jnp.dot(proj_b_w[...], x_buf[h * half_rows + k * half_rows // 2:h * half_rows + (k + 1) * half_rows // 2, lanes],
                       preferred_element_type=F32) + bias for k in range(2)]
        for d in range(hid):
            rows = jnp.concatenate([part[d * 8:(d + 1) * 8, :] for part in res], axis=0).astype(BF16)
            for at in range(lanes.start, lanes.stop, LANES):
                k = at // half_seq
                bt[slot_of(own, 0, h), k, d * HALF:(d + 1) * HALF, at - k * half_seq:at - k * half_seq + LANES] = (
                    rows[:, at - lanes.start:at - lanes.start + LANES])

    for p, group in enumerate(FIRST_OWN):
        for k in range(2):
            x_copies[2 * p + k].wait()
            norm_part(*parts[2 * p + k])
        if p == 0:
            for copy in x_copies[6:] + small[4:] + [z_copy]:
                copy.start()
        project_b(0, parts[2 * p][1])
        if p == 0:
            pl.semaphore_wait(barrier, 3)
        to_right(own, 0, 0, group)
        to_left(own, 0, 0, group)
    to_sib(own, 0, 0, ALL)
    for k in range(2):
        x_copies[6 + k].wait()
        norm_part(*parts[6 + k])
    project_b(1, parts[6][1])
    for group in SECOND_OWN:
        to_right(own, 0, 1, group)
        to_left(own, 0, 1, group)
    to_sib(own, 0, 1, ALL)

    for copy in small[4:]:
        copy.wait()
    row_bc[...] = column_lanes(ba_v[...].astype(F32).reshape(1, hid), hid)
    bias_a[...] = jnp.concatenate([row_bc[...]] * 4, axis=0)
    wa_rows = wa_v[...].astype(F32)
    wa_wide = jnp.concatenate([jnp.concatenate([wa_rows] * 4, axis=1)] * 4, axis=0)
    same = (iota(wa_wide.shape, 0) // hid) == (iota(wa_wide.shape, 1) // m_dim)
    proj_a_w[...] = jnp.where(same, wa_wide, 0.0).astype(BF16)
    for g in range(n_loc // 4):
        res = jnp.dot(proj_a_w[...], x_buf[g * 4 * m_dim:(g + 1) * 4 * m_dim, :], preferred_element_type=F32)
        res = res + jnp.concatenate([bias_a[...]] * (n_seq // LANES), axis=1)
        a_mat[:, g * LANES:(g + 1) * LANES] = res.T.astype(BF16)

    w_f32[...] = wo_v[...].astype(F32)
    w_diag[...] = jnp.zeros_like(w_diag)
    w_last[...] = jnp.zeros_like(w_last)

    def spread_w(d, at):
        block = w_f32[pl.ds(d, hid, stride=hid), :].astype(BF16)
        for k in range(4):
            row = pl.multiple_of(lax.rem(d, 8) * LANES + k * hid, hid)
            at[pl.ds(row, hid), k * LANES:(k + 1) * LANES] = block

    for c in range(PIECES):
        at = w_diag.at[c] if c < PIECES - 1 else w_last

        def body(d, carry):
            spread_w(d, at)
            return carry

        lax.fori_loop(c * 8, (c + 1) * 8, body, 0)

    def outer_piece(slot, c):
        rows = slice(c * BLOCK, (c + 1) * BLOCK)
        lhs = jnp.concatenate([bt[slot, 0, rows, :], bt[slot, 1, rows, :]], axis=1)
        res = jnp.dot(lhs, a_mat[...], preferred_element_type=F32)
        res = (res * inv_seq).astype(BF16)
        for d in range(8):
            for g in range(8):
                o_mat[c, g * HALF:(g + 1) * HALF, d * LANES:(d + 1) * LANES] = (
                    res[d * HALF:(d + 1) * HALF, g * LANES:(g + 1) * LANES])

    def project_piece(c):
        return jnp.dot(o_mat[c], w_diag[c] if c < PIECES - 1 else w_last[...], preferred_element_type=F32)

    chip = me // 2

    def column_of(q, r, h):
        src = lax.rem(chip + r, n_dev // 2) * 2 + q
        return pl.multiple_of(src * (2 * HALF) + h * HALF, HALF)

    bias_out = bo_v[...].astype(F32).reshape(1, LANES)

    def finish(update, bias, q, r, h):
        cols = pl.ds(column_of(q, r, h), HALF)
        for g in range(8):
            for k in range(4):
                i = g * 4 + k
                part = update[g * HALF:(g + 1) * HALF, k * LANES:(k + 1) * LANES]
                if bias is not None:
                    part = part + bias
                z_buf[i, cols, :] = (z_buf[i, cols, :].astype(F32) + part).astype(BF16)

    def half_unit(q, r, h):
        slot = slot_of(q, r, h)
        for c in range(PIECES):
            outer_piece(slot, c)
        update = project_piece(0)
        for c in range(1, PIECES):
            update = update + project_piece(c)
        finish(update, bias_out, q, r, h)

    z_copy.wait()
    for h in range(2):
        half_unit(own, 0, h)
    for h in range(2):
        arrived(other, 0, h, ALL)
        half_unit(other, 0, h)
    for h in range(2):
        for k, group in enumerate(SECOND_OWN if h else FIRST_OWN):
            arrived(own, 3, h, group)
            arrived(own, 1, h, group)
            if h == 1:
                to_left(own, 1, 1, SHARED[k])
        if h == 0:
            for group in SHARED:
                to_right(own, 3, 0, group)
        for r in (3, 1):
            to_sib(own, r, h, ALL)
        for r in (3, 1):
            half_unit(own, r, h)
        for r in (3, 1):
            arrived(other, r, h, ALL)

        @pl.when(core == 1)
        def _():
            for q in range(2):
                if h == 0:
                    to_right(q, 3, 0, FINAL)
                else:
                    to_left(q, 1, 1, FINAL)

        for r in (3, 1):
            half_unit(other, r, h)

    def pair_update(q, c):
        rows = slice(c * BLOCK, (c + 1) * BLOCK)
        lhs = [jnp.concatenate([bt[slot_of(q, 2, h), k, rows, :] for k in range(2)], axis=1) for h in range(2)]
        return pair_product(lhs, a_mat, w_diag[c] if c < PIECES - 1 else w_last[...], inv_seq)

    for h in range(2):
        arrived(own, 2, h, SHARED[0])
        to_sib(own, 2, h, SHARED[0])
    for q in (own, other):
        if q is other:
            for h in range(2):
                arrived(other, 2, h, SHARED[0])
        u_last[q] = pair_update(q, 0) + pair_update(q, 1) + jnp.concatenate([bias_out] * 4, axis=1)
    for h in range(2):
        arrived(own, 2, h, SHARED[1])
        to_sib(own, 2, h, SHARED[1])
    u_last[own] = u_last[own] + pair_update(own, 2)
    for h in range(2):
        arrived(0, 2, h, FINAL)

        @pl.when(core == 1)
        def _():
            to_sib(0, 2, h, FINAL)

    for h in range(2):
        arrived(other, 2, h, SHARED[1])
    u_last[other] = u_last[other] + pair_update(other, 2)

    @pl.when(core == 1)
    def _():
        for h in range(2):
            arrived(1, 2, h, FINAL)
            to_sib(1, 2, h, FINAL)

    update = u_last[0] + pair_update(0, PIECES - 1)
    for h in range(2):
        finish(update[h * BLOCK:(h + 1) * BLOCK, :], None, 0, 2, h)

    @pl.when(core == 0)
    def _():
        for h in range(2):
            arrived(1, 2, h, FINAL)

    for q, slots in enumerate((13, 15)):
        @pl.when(core == q)
        def _():
            everything = bt.at[pl.ds(0, slots)]
            pltpu.make_async_remote_copy(src_ref=everything, dst_ref=everything, send_sem=send_sem, recv_sem=recv_sem.at[0],
                                         device_id={'dap': sib}, device_id_type=MESH).wait_send()


def last_kernel(n_dev, z_buf, a_mat, w_last, u_last, bt_last, out_hbm, cols_buf, sem):
    width = 2 * HALF
    inv_seq = 1.0 / a_mat.shape[0]
    me = lax.axis_index('dap')
    chips = n_dev // 2
    mine = lax.rem(me // 2 + 2, chips) * 2 + 1

    def block(k):
        return pl.ds(pl.multiple_of(lax.rem(mine + k, n_dev) * width, width), width)

    copies = [pltpu.make_async_copy(z_buf.at[:, block(k), :], out_hbm.at[:, block(k), :], sem.at[k]) for k in range(1, n_dev)]
    for copy in copies:
        copy.start()
    lhs = [jnp.concatenate([bt_last[h, 0], bt_last[h, 1]], axis=1) for h in range(2)]
    update = u_last[1] + pair_product(lhs, a_mat, w_last[...], inv_seq)
    for h in range(2):
        cols = pl.ds(pl.multiple_of(mine * width + h * HALF, HALF), HALF)
        for g in range(8):
            for k in range(4):
                i = g * 4 + k
                lanes = slice(k * LANES, (k + 1) * LANES)
                part = update[h * BLOCK + g * HALF:h * BLOCK + (g + 1) * HALF, lanes]
                cols_buf[i, h * HALF:(h + 1) * HALF, :] = (z_buf[i, cols, :].astype(F32) + part).astype(BF16)
    copy = pltpu.make_async_copy(cols_buf, out_hbm.at[:, block(0), :], sem.at[0])
    copy.start()
    copies.append(copy)
    for copy in copies:
        copy.wait()


def solution(mesh):
    row_spec = P(('batch', 'dap'))
    col_spec = P(None, ('batch', 'dap'))
    rep_spec = P()
    n_dev = mesh.shape['dap']

    def local_update(z_rows, msa, ln_scale, ln_offset, w_a, b_a, w_b, b_b, w_out, b_out):
        n_seq, n_loc, m_dim = msa.shape
        hid = w_a.shape[1]
        pair = z_rows.shape[2]
        x = jnp.transpose(msa, (1, 2, 0)).reshape(n_loc * m_dim, n_seq)
        any_spec = pl.BlockSpec(memory_space=pltpu.HBM)
        vmem = pltpu.VMEM
        dma = pltpu.SemaphoreType.DMA
        outs = [
            vmem(z_rows.shape, BF16), vmem((n_seq, n_loc * hid), BF16), vmem((8 * LANES, 4 * pair), BF16),
            vmem((2, 2 * BLOCK, 4 * pair), F32), vmem((2, 2, BLOCK, n_seq // 2), BF16),
        ]
        vmem_spec = pl.BlockSpec(memory_space=pltpu.VMEM)
        made = pl.pallas_call(
            functools.partial(kernel, n_dev),
            out_shape=outs,
            in_specs=[any_spec] * 10,
            out_specs=[vmem_spec] * len(outs),
            scratch_shapes=[
                vmem(x.shape, BF16),
                vmem((m_dim,), BF16), vmem((m_dim,), BF16),
                vmem((hid, m_dim), BF16), vmem((hid,), BF16), vmem((hid, m_dim), BF16), vmem((hid,), BF16),
                vmem(w_out.shape, BF16), vmem((pair,), BF16),
                vmem((m_dim, LANES), F32), vmem((m_dim, LANES), F32),
                vmem((4 * hid, LANES), F32), vmem((8 * hid, LANES), F32), vmem((hid, LANES), F32),
                vmem((4 * hid, 4 * m_dim), BF16), vmem((8 * hid, 8 * m_dim), BF16),
                vmem((16, 2, PIECES * BLOCK, n_seq // 2), BF16),
                vmem((PIECES, LANES, 8 * LANES), BF16),
                vmem(w_out.shape, F32), vmem((PIECES - 1, 8 * LANES, 4 * pair), BF16),
                dma((8,)), dma((8,)), dma, dma((36,)), dma,
            ],
            compiler_params=pltpu.CompilerParams(collective_id=0, has_side_effects=True, vmem_limit_bytes=54 * 1024 * 1024),
            name='outer_mean_ring',
        )(*[pltpu.with_memory_space_constraint(part, pltpu.HBM)
            for part in (z_rows, x, ln_scale, ln_offset, w_a.T, b_a, w_b.T, b_b, w_out, b_out)])
        made = [pltpu.with_memory_space_constraint(part, pltpu.VMEM) for part in made]
        return pl.pallas_call(
            functools.partial(last_kernel, n_dev),
            out_shape=jax.ShapeDtypeStruct(z_rows.shape, BF16),
            in_specs=[vmem_spec] * len(outs),
            out_specs=any_spec,
            scratch_shapes=[vmem((n_loc, 2 * HALF, pair), BF16), dma((n_dev,))],
            compiler_params=pltpu.CompilerParams(vmem_limit_bytes=8 * 1024 * 1024),
            name='outer_mean_last',
        )(*made)

    return jax.shard_map(local_update, mesh=mesh, in_specs=(row_spec, col_spec) + (rep_spec,) * 8, out_specs=row_spec, check_vma=False)
```

```python
import functools

import jax
import jax.numpy as jnp
from jax import lax
from jax.experimental import pallas as pl
from jax.experimental.pallas import tpu as pltpu
from jax.sharding import PartitionSpec as P

LN_EPS = 1e-5
F32 = jnp.float32
BF16 = jnp.bfloat16
LANES = 128
HALF = 16
PIECES = 4
BLOCK = 128
ALL = ('rows', 0, 4)
FIRST_OWN = (('lanes', 0, 128), ('lanes', 128, 256), ('lanes', 256, 512))
SECOND_OWN = (('rows', 0, 2), ('rows', 2, 4))
SHARED = (('rows', 0, 2), ('rows', 2, 3))
FINAL = ('rows', 3, 4)
CLOSING = (('rows', 3, 3.5), ('rows', 3.5, 4))
MESH = pl.DeviceIdType.MESH


def iota(shape, dim):
    return lax.broadcasted_iota(jnp.int32, shape, dim)


def column_lanes(row, count):
    spread = jnp.broadcast_to(row, (count, count))
    picked = jnp.where(iota((count, count), 0) == iota((count, count), 1), spread, 0.0)
    return jnp.broadcast_to(jnp.sum(picked, axis=1, keepdims=True), (count, LANES))


def pair_product(lhs, a_mat, w_part, inv_seq):
    res = jnp.dot(jnp.concatenate(lhs, axis=0), a_mat[...], preferred_element_type=F32)
    res = (res * inv_seq).astype(BF16)
    size = lhs[0].shape[0]
    wide = jnp.concatenate(
        [jnp.concatenate([res[at:at + HALF, g * LANES:(g + 1) * LANES] for at in range(h * size, (h + 1) * size, HALF)], axis=1)
         for h in range(2) for g in range(8)], axis=0)
    return jnp.dot(wide, w_part, preferred_element_type=F32)


def kernel(n_dev, z_hbm, x_hbm, ls_hbm, lo_hbm, wa_hbm, ba_hbm, wb_hbm, bb_hbm, wo_hbm, bo_hbm,
           z_buf, a_mat, w_last, u_last, bt_last,
           x_buf, ls_v, lo_v, wa_v, ba_v, wb_v, bb_v, wo_v, bo_v,
           scale_bc, offset_bc, bias_a, bias_b, row_bc, proj_a_w, proj_b_w, bt, o_mat, w_f32, w_diag,
           small_sem, x_sem, z_sem, recv_sem, send_sem):
    n_seq = x_hbm.shape[1]
    n_loc = z_hbm.shape[0]
    m_dim = wa_hbm.shape[1]
    hid = wa_hbm.shape[0]
    inv_seq = 1.0 / n_seq
    me = lax.axis_index('dap')
    core = lax.rem(me, 2)
    sib = me + 1 - 2 * core
    right = lax.rem(me + 2, n_dev)
    left = lax.rem(me + n_dev - 2, n_dev)

    barrier = pltpu.get_barrier_semaphore()
    for peer in (sib, right, left):
        pl.semaphore_signal(barrier, inc=1, device_id={'dap': peer}, device_id_type=MESH)

    small = [pltpu.make_async_copy(src, dst, small_sem.at[k]) for k, (src, dst) in enumerate((
        (wb_hbm, wb_v), (bb_hbm, bb_v), (ls_hbm, ls_v), (lo_hbm, lo_v), (wa_hbm, wa_v), (ba_hbm, ba_v),
        (wo_hbm, wo_v), (bo_hbm, bo_v)))]
    half_rows = HALF * m_dim
    half_seq = n_seq // 2
    parts = [(slice(k * half_rows // 2, (k + 1) * half_rows // 2), slice(*group[1:]))
             for group in FIRST_OWN for k in range(2)]
    parts += [(slice(half_rows + k * half_rows // 2, half_rows + (k + 1) * half_rows // 2), slice(0, n_seq)) for k in range(2)]
    x_copies = [pltpu.make_async_copy(x_hbm.at[part], x_buf.at[part], x_sem.at[k]) for k, part in enumerate(parts)]
    for copy in small[:4] + x_copies[:6]:
        copy.start()
    z_copy = pltpu.make_async_copy(z_hbm, z_buf, z_sem)

    for copy in small[:4]:
        copy.wait()
    row_bc[...] = column_lanes(bb_v[...].astype(F32).reshape(1, hid), hid)
    wb_rows = wb_v[...].astype(F32)
    wb_two = jnp.concatenate([wb_rows, wb_rows], axis=1)
    scale_bc[...] = column_lanes(ls_v[...].astype(F32).reshape(1, m_dim), m_dim)
    offset_bc[...] = column_lanes(lo_v[...].astype(F32).reshape(1, m_dim), m_dim)
    in_eight = iota((8, LANES), 0)
    in_pair = iota((8, LANES), 1) // m_dim
    for d in range(0, hid, 2):
        for t in range(8 * m_dim // LANES):
            part = [jnp.where(in_eight == in_pair + 2 * t, jnp.broadcast_to(wb_two[e:e + 1, :], (8, LANES)), 0.0)
                    for e in (d, d + 1)]
            proj_b_w[d * 8:(d + 2) * 8, t * LANES:(t + 1) * LANES] = jnp.concatenate(part, axis=0).astype(BF16)
        for e in (d, d + 1):
            bias_b[e * 8:(e + 1) * 8, :] = jnp.broadcast_to(row_bc[e:e + 1, :], (8, LANES))

    def norm_part(rows, lanes):
        width = lanes.stop - lanes.start
        scale = jnp.concatenate([scale_bc[...]] * (width // LANES), axis=1)
        offset = jnp.concatenate([offset_bc[...]] * (width // LANES), axis=1)

        def body(n, carry):
            at = (pl.ds(pl.multiple_of(rows.start + n * m_dim, m_dim), m_dim), lanes)
            value = x_buf[at].astype(F32)
            mean = jnp.sum(value, axis=0, keepdims=True) * (1.0 / m_dim)
            centred = value - mean
            var = jnp.sum(centred * centred, axis=0, keepdims=True) * (1.0 / m_dim)
            normed = centred * lax.rsqrt(var + LN_EPS)
            x_buf[at] = (normed * scale + offset).astype(BF16)
            return carry

        lax.fori_loop(0, (rows.stop - rows.start) // m_dim, body, 0, unroll=8)

    def slot_of(q, r, h):
        return q * 8 + r * 2 + h

    def view(q, r, h, group):
        slot = slot_of(q, r, h)
        if group[0] == 'lanes':
            k = group[1] // half_seq
            return bt.at[slot, k, :, pl.ds(group[1] - k * half_seq, group[2] - group[1])]
        if group == ALL:
            return bt.at[slot]
        return bt.at[slot, :, pl.ds(int(group[1] * BLOCK), int((group[2] - group[1]) * BLOCK)), :]

    names = ['own first', 'own second r3', 'own second r1 0', 'own second r1 1', 'own shared 0', 'own shared 1', 'other r0',
             'other first', 'other second', 'other shared 0', 'other shared 1', 'final', 'closing 0', 'closing 1']

    def semaphore_name(mine, r, h, group):
        if group == FINAL:
            return 'final'
        if group in CLOSING:
            return f'closing {CLOSING.index(group)}'
        if r == 2:
            return ('own' if mine else 'other') + f' shared {SHARED.index(group)}'
        if not mine:
            return 'other r0' if r == 0 else 'other second' if h else 'other first'
        if h == 0:
            return 'own first'
        return 'own second r3' if r == 3 else f'own second r1 {SECOND_OWN.index(group)}'

    def transfer(src, dst, name, peer):
        return pltpu.make_async_remote_copy(
            src_ref=src, dst_ref=dst, send_sem=send_sem, recv_sem=recv_sem.at[names.index(name)], device_id={'dap': peer},
            device_id_type=MESH)

    def arrived(name, halves):
        if halves >= 1:
            shape = bt.at[pl.ds(0, halves)]
        else:
            shape = bt.at[pl.ds(0, 2), :, pl.ds(0, int(halves * PIECES * BLOCK) // 2)]
        transfer(shape, shape, name, sib).wait_recv()

    def to_right(q, r, h, group, mine=True):
        there = (r + 3) % 4
        transfer(view(q, r, h, group), view(q, there, h, group), semaphore_name(mine, there, h, group), right).start()

    def to_left(q, r, h, group, mine=True):
        there = (r + 1) % 4
        transfer(view(q, r, h, group), view(q, there, h, group), semaphore_name(mine, there, h, group), left).start()

    def to_sib(q, r, h, group):
        dst = bt_last.at[h] if group == CLOSING[1] else view(q, r, h, group)
        transfer(view(q, r, h, group), dst, semaphore_name(False, r, h, group), sib).start()

    own, other = core, 1 - core

    def project_b(h, lanes):
        width = lanes.stop - lanes.start
        bias = jnp.concatenate([bias_b[...]] * (width // LANES), axis=1)
        res = [jnp.dot(proj_b_w[...], x_buf[h * half_rows + k * half_rows // 2:h * half_rows + (k + 1) * half_rows // 2, lanes],
                       preferred_element_type=F32) + bias for k in range(2)]
        for d in range(hid):
            rows = jnp.concatenate([part[d * 8:(d + 1) * 8, :] for part in res], axis=0).astype(BF16)
            for at in range(lanes.start, lanes.stop, LANES):
                k = at // half_seq
                bt[slot_of(own, 0, h), k, d * HALF:(d + 1) * HALF, at - k * half_seq:at - k * half_seq + LANES] = (
                    rows[:, at - lanes.start:at - lanes.start + LANES])

    for p, group in enumerate(FIRST_OWN):
        for k in range(2):
            x_copies[2 * p + k].wait()
            norm_part(*parts[2 * p + k])
        if p == 0:
            for copy in x_copies[6:] + small[4:] + [z_copy]:
                copy.start()
        project_b(0, parts[2 * p][1])
        if p == 0:
            pl.semaphore_wait(barrier, 3)
        to_right(own, 0, 0, group)
        to_left(own, 0, 0, group)
    to_sib(own, 0, 0, ALL)
    for k in range(2):
        x_copies[6 + k].wait()
        norm_part(*parts[6 + k])
    project_b(1, parts[6][1])
    for group in SECOND_OWN:
        to_right(own, 0, 1, group)
        to_left(own, 0, 1, group)
    to_sib(own, 0, 1, ALL)

    for copy in small[4:]:
        copy.wait()
    row_bc[...] = column_lanes(ba_v[...].astype(F32).reshape(1, hid), hid)
    bias_a[...] = jnp.concatenate([row_bc[...]] * 4, axis=0)
    wa_rows = wa_v[...].astype(F32)
    wa_wide = jnp.concatenate([jnp.concatenate([wa_rows] * 4, axis=1)] * 4, axis=0)
    same = (iota(wa_wide.shape, 0) // hid) == (iota(wa_wide.shape, 1) // m_dim)
    proj_a_w[...] = jnp.where(same, wa_wide, 0.0).astype(BF16)
    for g in range(n_loc // 4):
        res = jnp.dot(proj_a_w[...], x_buf[g * 4 * m_dim:(g + 1) * 4 * m_dim, :], preferred_element_type=F32)
        res = res + jnp.concatenate([bias_a[...]] * (n_seq // LANES), axis=1)
        a_mat[:, g * LANES:(g + 1) * LANES] = res.T.astype(BF16)

    w_f32[...] = wo_v[...].astype(F32)
    w_diag[...] = jnp.zeros_like(w_diag)
    w_last[...] = jnp.zeros_like(w_last)

    def spread_w(d, at):
        block = w_f32[pl.ds(d, hid, stride=hid), :].astype(BF16)
        for k in range(4):
            row = pl.multiple_of(lax.rem(d, 8) * LANES + k * hid, hid)
            at[pl.ds(row, hid), k * LANES:(k + 1) * LANES] = block

    for c in range(PIECES):
        at = w_diag.at[c] if c < PIECES - 1 else w_last

        def body(d, carry):
            spread_w(d, at)
            return carry

        lax.fori_loop(c * 8, (c + 1) * 8, body, 0)

    def outer_piece(slot, c):
        rows = slice(c * BLOCK, (c + 1) * BLOCK)
        lhs = jnp.concatenate([bt[slot, 0, rows, :], bt[slot, 1, rows, :]], axis=1)
        res = jnp.dot(lhs, a_mat[...], preferred_element_type=F32)
        res = (res * inv_seq).astype(BF16)
        for d in range(8):
            for g in range(8):
                o_mat[c, g * HALF:(g + 1) * HALF, d * LANES:(d + 1) * LANES] = (
                    res[d * HALF:(d + 1) * HALF, g * LANES:(g + 1) * LANES])

    def project_piece(c):
        return jnp.dot(o_mat[c], w_diag[c] if c < PIECES - 1 else w_last[...], preferred_element_type=F32)

    chip = me // 2

    def column_of(q, r, h):
        src = lax.rem(chip + r, n_dev // 2) * 2 + q
        return pl.multiple_of(src * (2 * HALF) + h * HALF, HALF)

    bias_out = bo_v[...].astype(F32).reshape(1, LANES)

    def finish(update, bias, q, r, h):
        cols = pl.ds(column_of(q, r, h), HALF)
        for g in range(8):
            for k in range(4):
                i = g * 4 + k
                part = update[g * HALF:(g + 1) * HALF, k * LANES:(k + 1) * LANES]
                if bias is not None:
                    part = part + bias
                z_buf[i, cols, :] = (z_buf[i, cols, :].astype(F32) + part).astype(BF16)

    def half_unit(q, r, h):
        slot = slot_of(q, r, h)
        for c in range(PIECES):
            outer_piece(slot, c)
        update = project_piece(0)
        for c in range(1, PIECES):
            update = update + project_piece(c)
        finish(update, bias_out, q, r, h)

    z_copy.wait()
    for h in range(2):
        half_unit(own, 0, h)
    arrived('other r0', 2)
    for h in range(2):
        half_unit(other, 0, h)
    for h in range(2):
        if h == 0:
            arrived('own first', 2)
            for group in SHARED:
                to_right(own, 3, 0, group)
        else:
            for k in range(2):
                arrived(f'own second r1 {k}', 0.5)
                to_left(own, 1, 1, SHARED[k])
            arrived('own second r3', 1)
        for r in (3, 1):
            to_sib(own, r, h, ALL)
        for r in (3, 1):
            half_unit(own, r, h)
        arrived('other second' if h else 'other first', 2)

        @pl.when(core == 1)
        def _():
            for q, groups in ((0, (FINAL,)), (1, CLOSING)):
                for group in groups:
                    if h == 0:
                        to_right(q, 3, 0, group)
                    else:
                        to_left(q, 1, 1, group)

        for r in (3, 1):
            half_unit(other, r, h)

    def pair_update(q, group):
        rows = slice(int(group[1] * BLOCK), int(group[2] * BLOCK))
        lhs = [jnp.concatenate([bt[slot_of(q, 2, h), k, rows, :] for k in range(2)], axis=1) for h in range(2)]
        c = int(group[1])
        at = slice(int((group[1] - c) * 8 * LANES), int((group[2] - c) * 8 * LANES))
        return pair_product(lhs, a_mat, w_diag[c, at, :] if c < PIECES - 1 else w_last[at, :], inv_seq)

    def finish_pair(update, q):
        for h in range(2):
            finish(update[h * BLOCK:(h + 1) * BLOCK, :], None, q, 2, h)

    first_pieces = (('rows', 0, 1), ('rows', 1, 2))
    for q in (own, other):
        arrived('own shared 0' if q is own else 'other shared 0', 1)
        if q is own:
            for h in range(2):
                to_sib(own, 2, h, SHARED[0])
        u_last[q] = pair_update(q, first_pieces[0]) + pair_update(q, first_pieces[1]) + jnp.concatenate([bias_out] * 4, axis=1)
    arrived('own shared 1', 0.5)
    for h in range(2):
        to_sib(own, 2, h, SHARED[1])
    u_last[own] = u_last[own] + pair_update(own, SHARED[1])

    @pl.when(core == 1)
    def _():
        arrived('final', 0.5)
        for h in range(2):
            to_sib(0, 2, h, FINAL)
        u_last[0] = u_last[0] + pair_update(0, FINAL)
        arrived('closing 0', 0.25)
        for h in range(2):
            to_sib(1, 2, h, CLOSING[0])
        arrived('other shared 1', 0.5)
        u_last[0] = u_last[0] + pair_update(0, SHARED[1])
        arrived('closing 1', 0.25)
        for h in range(2):
            to_sib(1, 2, h, CLOSING[1])
        finish_pair(u_last[0], 0)
        finish_pair(u_last[1] + pair_update(1, FINAL), 1)

    @pl.when(core == 0)
    def _():
        arrived('other shared 1', 0.5)
        u_last[1] = u_last[1] + pair_update(1, SHARED[1])
        arrived('final', 0.5)
        finish_pair(u_last[0] + pair_update(0, FINAL), 0)
        arrived('closing 0', 0.25)
        u_last[1] = u_last[1] + pair_update(1, CLOSING[0])
        arrived('closing 1', 0.25)

    for q, slots in enumerate((13, 15)):
        @pl.when(core == q)
        def _():
            everything = bt.at[pl.ds(0, slots)]
            pltpu.make_async_remote_copy(src_ref=everything, dst_ref=everything, send_sem=send_sem, recv_sem=recv_sem.at[0],
                                         device_id={'dap': sib}, device_id_type=MESH).wait_send()


def last_kernel(n_dev, z_buf, a_mat, w_last, u_last, bt_last, out_hbm, cols_buf, sem):
    width = 2 * HALF
    inv_seq = 1.0 / a_mat.shape[0]
    me = lax.axis_index('dap')
    chips = n_dev // 2
    mine = lax.rem(me // 2 + 2, chips) * 2 + 1

    def block(k):
        return pl.ds(pl.multiple_of(lax.rem(mine + k, n_dev) * width, width), width)

    core = lax.rem(me, 2)
    copies = [pltpu.make_async_copy(z_buf.at[:, block(k), :], out_hbm.at[:, block(k), :], sem.at[k]) for k in range(n_dev)]
    for copy in copies[1:]:
        copy.start()

    @pl.when(core == 1)
    def _():
        copies[0].start()

    @pl.when(core == 0)
    def _():
        lhs = [jnp.concatenate([bt_last[h, 0], bt_last[h, 1]], axis=1) for h in range(2)]
        rows = lhs[0].shape[0] * 8
        update = u_last[1] + pair_product(lhs, a_mat, w_last[w_last.shape[0] - rows:, :], inv_seq)
        for h in range(2):
            cols = pl.ds(pl.multiple_of(mine * width + h * HALF, HALF), HALF)
            for g in range(8):
                for k in range(4):
                    i = g * 4 + k
                    part = update[h * BLOCK + g * HALF:h * BLOCK + (g + 1) * HALF, k * LANES:(k + 1) * LANES]
                    cols_buf[i, h * HALF:(h + 1) * HALF, :] = (z_buf[i, cols, :].astype(F32) + part).astype(BF16)
        pltpu.make_async_copy(cols_buf, out_hbm.at[:, block(0), :], sem.at[0]).start()

    for copy in copies:
        copy.wait()


def solution(mesh):
    row_spec = P(('batch', 'dap'))
    col_spec = P(None, ('batch', 'dap'))
    rep_spec = P()
    n_dev = mesh.shape['dap']

    def local_update(z_rows, msa, ln_scale, ln_offset, w_a, b_a, w_b, b_b, w_out, b_out):
        n_seq, n_loc, m_dim = msa.shape
        hid = w_a.shape[1]
        pair = z_rows.shape[2]
        x = jnp.transpose(msa, (1, 2, 0)).reshape(n_loc * m_dim, n_seq)
        any_spec = pl.BlockSpec(memory_space=pltpu.HBM)
        vmem = pltpu.VMEM
        dma = pltpu.SemaphoreType.DMA
        outs = [
            vmem(z_rows.shape, BF16), vmem((n_seq, n_loc * hid), BF16), vmem((8 * LANES, 4 * pair), BF16),
            vmem((2, 2 * BLOCK, 4 * pair), F32), vmem((2, 2, BLOCK // 2, n_seq // 2), BF16),
        ]
        vmem_spec = pl.BlockSpec(memory_space=pltpu.VMEM)
        made = pl.pallas_call(
            functools.partial(kernel, n_dev),
            out_shape=outs,
            in_specs=[any_spec] * 10,
            out_specs=[vmem_spec] * len(outs),
            scratch_shapes=[
                vmem(x.shape, BF16),
                vmem((m_dim,), BF16), vmem((m_dim,), BF16),
                vmem((hid, m_dim), BF16), vmem((hid,), BF16), vmem((hid, m_dim), BF16), vmem((hid,), BF16),
                vmem(w_out.shape, BF16), vmem((pair,), BF16),
                vmem((m_dim, LANES), F32), vmem((m_dim, LANES), F32),
                vmem((4 * hid, LANES), F32), vmem((8 * hid, LANES), F32), vmem((hid, LANES), F32),
                vmem((4 * hid, 4 * m_dim), BF16), vmem((8 * hid, 8 * m_dim), BF16),
                vmem((16, 2, PIECES * BLOCK, n_seq // 2), BF16),
                vmem((PIECES, LANES, 8 * LANES), BF16),
                vmem(w_out.shape, F32), vmem((PIECES - 1, 8 * LANES, 4 * pair), BF16),
                dma((8,)), dma((8,)), dma, dma((14,)), dma,
            ],
            compiler_params=pltpu.CompilerParams(collective_id=0, has_side_effects=True, vmem_limit_bytes=54 * 1024 * 1024),
            name='outer_mean_ring',
        )(*[pltpu.with_memory_space_constraint(part, pltpu.HBM)
            for part in (z_rows, x, ln_scale, ln_offset, w_a.T, b_a, w_b.T, b_b, w_out, b_out)])
        made = [pltpu.with_memory_space_constraint(part, pltpu.VMEM) for part in made]
        return pl.pallas_call(
            functools.partial(last_kernel, n_dev),
            out_shape=jax.ShapeDtypeStruct(z_rows.shape, BF16),
            in_specs=[vmem_spec] * len(outs),
            out_specs=any_spec,
            scratch_shapes=[vmem((n_loc, 2 * HALF, pair), BF16), dma((n_dev,))],
            compiler_params=pltpu.CompilerParams(vmem_limit_bytes=8 * 1024 * 1024),
            name='outer_mean_last',
        )(*made)

    return jax.shard_map(local_update, mesh=mesh, in_specs=(row_spec, col_spec) + (rep_spec,) * 8, out_specs=row_spec, check_vma=False)
```

```python
import functools

import jax
import jax.numpy as jnp
from jax import lax
from jax.experimental import pallas as pl
from jax.experimental.pallas import tpu as pltpu
from jax.sharding import PartitionSpec as P

LN_EPS = 1e-5
F32 = jnp.float32
BF16 = jnp.bfloat16
LANES = 128
HALF = 16
PIECES = 4
BLOCK = 128
ALL = ('rows', 0, 4)
FIRST_OWN = (('lanes', 0, 128), ('lanes', 128, 256), ('lanes', 256, 512))
SECOND_OWN = (('rows', 0, 2), ('rows', 2, 4))
SHARED = (('rows', 0, 1), ('rows', 1, 2), ('rows', 2, 3))
FINAL = ('rows', 3, 4)
CLOSING = (('rows', 3, 3.5), ('rows', 3.5, 4))
MESH = pl.DeviceIdType.MESH


def iota(shape, dim):
    return lax.broadcasted_iota(jnp.int32, shape, dim)


def column_lanes(row, count):
    spread = jnp.broadcast_to(row, (count, count))
    picked = jnp.where(iota((count, count), 0) == iota((count, count), 1), spread, 0.0)
    return jnp.broadcast_to(jnp.sum(picked, axis=1, keepdims=True), (count, LANES))


def pair_product(lhs, a_mat, w_part, inv_seq):
    res = jnp.dot(jnp.concatenate(lhs, axis=0), a_mat[...], preferred_element_type=F32)
    res = (res * inv_seq).astype(BF16)
    size = lhs[0].shape[0]
    wide = jnp.concatenate(
        [jnp.concatenate([res[at:at + HALF, g * LANES:(g + 1) * LANES] for at in range(h * size, (h + 1) * size, HALF)], axis=1)
         for h in range(2) for g in range(8)], axis=0)
    return jnp.dot(wide, w_part, preferred_element_type=F32)


def kernel(n_dev, z_hbm, x_hbm, ls_hbm, lo_hbm, wa_hbm, ba_hbm, wb_hbm, bb_hbm, wo_hbm, bo_hbm,
           z_buf, a_mat, w_last, u_last, bt_last,
           x_buf, ls_v, lo_v, wa_v, ba_v, wb_v, bb_v, wo_v, bo_v,
           scale_bc, offset_bc, bias_a, bias_b, row_bc, proj_a_w, proj_b_w, bt, o_mat, w_f32, w_diag,
           small_sem, x_sem, z_sem, recv_sem, send_sem):
    n_seq = x_hbm.shape[1]
    n_loc = z_hbm.shape[0]
    m_dim = wa_hbm.shape[1]
    hid = wa_hbm.shape[0]
    inv_seq = 1.0 / n_seq
    me = lax.axis_index('dap')
    core = lax.rem(me, 2)
    sib = me + 1 - 2 * core
    right = lax.rem(me + 2, n_dev)
    left = lax.rem(me + n_dev - 2, n_dev)

    barrier = pltpu.get_barrier_semaphore()
    for peer in (sib, right, left):
        pl.semaphore_signal(barrier, inc=1, device_id={'dap': peer}, device_id_type=MESH)

    small = [pltpu.make_async_copy(src, dst, small_sem.at[k]) for k, (src, dst) in enumerate((
        (wb_hbm, wb_v), (bb_hbm, bb_v), (ls_hbm, ls_v), (lo_hbm, lo_v), (wa_hbm, wa_v), (ba_hbm, ba_v),
        (wo_hbm, wo_v), (bo_hbm, bo_v)))]
    half_rows = HALF * m_dim
    half_seq = n_seq // 2
    parts = [(slice(k * half_rows // 2, (k + 1) * half_rows // 2), slice(*group[1:]))
             for group in FIRST_OWN for k in range(2)]
    parts += [(slice(half_rows + k * half_rows // 2, half_rows + (k + 1) * half_rows // 2), slice(0, n_seq)) for k in range(2)]
    x_copies = [pltpu.make_async_copy(x_hbm.at[part], x_buf.at[part], x_sem.at[k]) for k, part in enumerate(parts)]
    for copy in small[:4] + x_copies[:6]:
        copy.start()
    z_copy = pltpu.make_async_copy(z_hbm, z_buf, z_sem)

    for copy in small[:4]:
        copy.wait()
    row_bc[...] = column_lanes(bb_v[...].astype(F32).reshape(1, hid), hid)
    wb_rows = wb_v[...].astype(F32)
    wb_two = jnp.concatenate([wb_rows, wb_rows], axis=1)
    scale_bc[...] = column_lanes(ls_v[...].astype(F32).reshape(1, m_dim), m_dim)
    offset_bc[...] = column_lanes(lo_v[...].astype(F32).reshape(1, m_dim), m_dim)
    in_eight = iota((8, LANES), 0)
    in_pair = iota((8, LANES), 1) // m_dim
    for d in range(0, hid, 2):
        for t in range(8 * m_dim // LANES):
            part = [jnp.where(in_eight == in_pair + 2 * t, jnp.broadcast_to(wb_two[e:e + 1, :], (8, LANES)), 0.0)
                    for e in (d, d + 1)]
            proj_b_w[d * 8:(d + 2) * 8, t * LANES:(t + 1) * LANES] = jnp.concatenate(part, axis=0).astype(BF16)
        for e in (d, d + 1):
            bias_b[e * 8:(e + 1) * 8, :] = jnp.broadcast_to(row_bc[e:e + 1, :], (8, LANES))

    def norm_part(rows, lanes):
        width = lanes.stop - lanes.start
        scale = jnp.concatenate([scale_bc[...]] * (width // LANES), axis=1)
        offset = jnp.concatenate([offset_bc[...]] * (width // LANES), axis=1)

        def body(n, carry):
            at = (pl.ds(pl.multiple_of(rows.start + n * m_dim, m_dim), m_dim), lanes)
            value = x_buf[at].astype(F32)
            mean = jnp.sum(value, axis=0, keepdims=True) * (1.0 / m_dim)
            centred = value - mean
            var = jnp.sum(centred * centred, axis=0, keepdims=True) * (1.0 / m_dim)
            normed = centred * lax.rsqrt(var + LN_EPS)
            x_buf[at] = (normed * scale + offset).astype(BF16)
            return carry

        lax.fori_loop(0, (rows.stop - rows.start) // m_dim, body, 0, unroll=8)

    def slot_of(q, r, h):
        return q * 8 + r * 2 + h

    def view(q, r, h, group):
        slot = slot_of(q, r, h)
        if group[0] == 'lanes':
            k = group[1] // half_seq
            return bt.at[slot, k, :, pl.ds(group[1] - k * half_seq, group[2] - group[1])]
        if group == ALL:
            return bt.at[slot]
        return bt.at[slot, :, pl.ds(int(group[1] * BLOCK), int((group[2] - group[1]) * BLOCK)), :]

    names = ['own first', 'own second 0', 'own second 1', 'own shared 0', 'own shared 1', 'own shared 2', 'other r0',
             'other first', 'other second 0', 'other second 1', 'other shared 0', 'other shared 1', 'other shared 2', 'final', 'closing 0', 'closing 1']

    def semaphore_name(mine, r, h, group):
        if group == FINAL:
            return 'final'
        if group in CLOSING:
            return f'closing {CLOSING.index(group)}'
        if r == 2:
            return ('own' if mine else 'other') + f' shared {SHARED.index(group)}'
        if not mine:
            if r == 0:
                return 'other r0'
            return f'other second {SECOND_OWN.index(group)}' if h else 'other first'
        return f'own second {SECOND_OWN.index(group)}' if h else 'own first'

    def transfer(src, dst, name, peer):
        return pltpu.make_async_remote_copy(
            src_ref=src, dst_ref=dst, send_sem=send_sem, recv_sem=recv_sem.at[names.index(name)], device_id={'dap': peer},
            device_id_type=MESH)

    def arrived(name, halves):
        if halves >= 1:
            shape = bt.at[pl.ds(0, halves)]
        else:
            shape = bt.at[pl.ds(0, 2), :, pl.ds(0, int(halves * PIECES * BLOCK) // 2)]
        transfer(shape, shape, name, sib).wait_recv()

    def to_right(q, r, h, group, mine=True):
        there = (r + 3) % 4
        transfer(view(q, r, h, group), view(q, there, h, group), semaphore_name(mine, there, h, group), right).start()

    def to_left(q, r, h, group, mine=True):
        there = (r + 1) % 4
        transfer(view(q, r, h, group), view(q, there, h, group), semaphore_name(mine, there, h, group), left).start()

    def to_sib(q, r, h, group):
        dst = bt_last.at[h] if group == CLOSING[1] else view(q, r, h, group)
        transfer(view(q, r, h, group), dst, semaphore_name(False, r, h, group), sib).start()

    own, other = core, 1 - core

    def project_b(h, lanes):
        width = lanes.stop - lanes.start
        bias = jnp.concatenate([bias_b[...]] * (width // LANES), axis=1)
        res = [jnp.dot(proj_b_w[...], x_buf[h * half_rows + k * half_rows // 2:h * half_rows + (k + 1) * half_rows // 2, lanes],
                       preferred_element_type=F32) + bias for k in range(2)]
        for d in range(hid):
            rows = jnp.concatenate([part[d * 8:(d + 1) * 8, :] for part in res], axis=0).astype(BF16)
            for at in range(lanes.start, lanes.stop, LANES):
                k = at // half_seq
                bt[slot_of(own, 0, h), k, d * HALF:(d + 1) * HALF, at - k * half_seq:at - k * half_seq + LANES] = (
                    rows[:, at - lanes.start:at - lanes.start + LANES])

    for p, group in enumerate(FIRST_OWN):
        for k in range(2):
            x_copies[2 * p + k].wait()
            norm_part(*parts[2 * p + k])
        if p == 0:
            for copy in x_copies[6:] + small[4:] + [z_copy]:
                copy.start()
        project_b(0, parts[2 * p][1])
        if p == 0:
            pl.semaphore_wait(barrier, 3)
        to_right(own, 0, 0, group)
        to_left(own, 0, 0, group)
    to_sib(own, 0, 0, ALL)
    for k in range(2):
        x_copies[6 + k].wait()
        norm_part(*parts[6 + k])
    project_b(1, parts[6][1])
    for group in SECOND_OWN:
        to_right(own, 0, 1, group)
        to_left(own, 0, 1, group)
    to_sib(own, 0, 1, ALL)

    for copy in small[4:]:
        copy.wait()
    row_bc[...] = column_lanes(ba_v[...].astype(F32).reshape(1, hid), hid)
    bias_a[...] = jnp.concatenate([row_bc[...]] * 4, axis=0)
    wa_rows = wa_v[...].astype(F32)
    wa_wide = jnp.concatenate([jnp.concatenate([wa_rows] * 4, axis=1)] * 4, axis=0)
    same = (iota(wa_wide.shape, 0) // hid) == (iota(wa_wide.shape, 1) // m_dim)
    proj_a_w[...] = jnp.where(same, wa_wide, 0.0).astype(BF16)
    for g in range(n_loc // 4):
        res = jnp.dot(proj_a_w[...], x_buf[g * 4 * m_dim:(g + 1) * 4 * m_dim, :], preferred_element_type=F32)
        res = res + jnp.concatenate([bias_a[...]] * (n_seq // LANES), axis=1)
        a_mat[:, g * LANES:(g + 1) * LANES] = res.T.astype(BF16)

    w_f32[...] = wo_v[...].astype(F32)
    w_diag[...] = jnp.zeros_like(w_diag)
    w_last[...] = jnp.zeros_like(w_last)

    def spread_w(d, at):
        block = w_f32[pl.ds(d, hid, stride=hid), :].astype(BF16)
        for k in range(4):
            row = pl.multiple_of(lax.rem(d, 8) * LANES + k * hid, hid)
            at[pl.ds(row, hid), k * LANES:(k + 1) * LANES] = block

    for c in range(PIECES):
        at = w_diag.at[c] if c < PIECES - 1 else w_last

        def body(d, carry):
            spread_w(d, at)
            return carry

        lax.fori_loop(c * 8, (c + 1) * 8, body, 0)

    def outer_piece(slot, c):
        rows = slice(c * BLOCK, (c + 1) * BLOCK)
        lhs = jnp.concatenate([bt[slot, 0, rows, :], bt[slot, 1, rows, :]], axis=1)
        res = jnp.dot(lhs, a_mat[...], preferred_element_type=F32)
        res = (res * inv_seq).astype(BF16)
        for d in range(8):
            for g in range(8):
                o_mat[c, g * HALF:(g + 1) * HALF, d * LANES:(d + 1) * LANES] = (
                    res[d * HALF:(d + 1) * HALF, g * LANES:(g + 1) * LANES])

    def project_piece(c):
        return jnp.dot(o_mat[c], w_diag[c] if c < PIECES - 1 else w_last[...], preferred_element_type=F32)

    chip = me // 2

    def column_of(q, r, h):
        src = lax.rem(chip + r, n_dev // 2) * 2 + q
        return pl.multiple_of(src * (2 * HALF) + h * HALF, HALF)

    bias_out = bo_v[...].astype(F32).reshape(1, LANES)

    def finish(update, bias, q, r, h):
        cols = pl.ds(column_of(q, r, h), HALF)
        for g in range(8):
            for k in range(4):
                i = g * 4 + k
                part = update[g * HALF:(g + 1) * HALF, k * LANES:(k + 1) * LANES]
                if bias is not None:
                    part = part + bias
                z_buf[i, cols, :] = (z_buf[i, cols, :].astype(F32) + part).astype(BF16)

    def half_unit(q, r, h):
        slot = slot_of(q, r, h)
        for c in range(PIECES):
            outer_piece(slot, c)
        update = project_piece(0)
        for c in range(1, PIECES):
            update = update + project_piece(c)
        finish(update, bias_out, q, r, h)

    z_copy.wait()
    for h in range(2):
        half_unit(own, 0, h)
    arrived('other r0', 2)
    for h in range(2):
        half_unit(other, 0, h)
    def pair_update(q, slots, group):
        rows = slice(int(group[1] * BLOCK), int(group[2] * BLOCK))
        lhs = [jnp.concatenate([bt[slot_of(q, r, h), k, rows, :] for k in range(2)], axis=1) for r, h in slots]
        c = int(group[1])
        at = slice(int((group[1] - c) * 8 * LANES), int((group[2] - c) * 8 * LANES))
        return pair_product(lhs, a_mat, w_diag[c, at, :] if c < PIECES - 1 else w_last[at, :], inv_seq)

    def finish_pair(update, q, slots):
        for k, (r, h) in enumerate(slots):
            finish(update[k * BLOCK:(k + 1) * BLOCK, :], None, q, r, h)

    far, near = ((2, 0), (2, 1)), ((3, 1), (1, 1))
    wide_bias = jnp.concatenate([bias_out] * 4, axis=1)

    def send_final(h):
        @pl.when(core == 1)
        def _():
            for q, groups in ((0, (FINAL,)), (1, CLOSING)):
                for group in groups:
                    if h == 0:
                        to_right(q, 3, 0, group)
                    else:
                        to_left(q, 1, 1, group)


    arrived('own first', 2)
    for group in SHARED:
        to_right(own, 3, 0, group)
    for r in (3, 1):
        to_sib(own, r, 0, ALL)
    for r in (3, 1):
        half_unit(own, r, 0)
    arrived('other first', 2)
    send_final(0)
    for r in (3, 1):
        half_unit(other, r, 0)
    for k, group in enumerate(SECOND_OWN):
        arrived(f'own second {k}', 1)
        for part in SHARED:
            if group[1] <= part[1] < group[2]:
                to_left(own, 1, 1, part)
        for r in (3, 1):
            to_sib(own, r, 1, group)
        blocks = [('rows', c, c + 1) for c in range(*group[1:])]
        for q in (own, other):
            if q is other:
                arrived(f'other second {k}', 1)
                if k == 1:
                    send_final(1)
            update = pair_update(q, near, blocks[0]) + pair_update(q, near, blocks[1])
            if k == 0:
                u_last[q] = update + wide_bias
            else:
                finish_pair(u_last[q] + update, q, near)

    for k, group in enumerate(SHARED):
        arrived(f'own shared {k}', 0.5)
        for h in range(2):
            to_sib(own, 2, h, group)
        for q in (own, other)[:2 if k < 2 else 1]:
            if q is other:
                arrived(f'other shared {k}', 0.5)
            update = pair_update(q, far, group)
            u_last[q] = u_last[q] + update if k else update + wide_bias

    @pl.when(core == 1)
    def _():
        arrived('final', 0.5)
        for h in range(2):
            to_sib(0, 2, h, FINAL)
        u_last[0] = u_last[0] + pair_update(0, far, FINAL)
        arrived('closing 0', 0.25)
        for h in range(2):
            to_sib(1, 2, h, CLOSING[0])
        arrived('other shared 2', 0.5)
        u_last[0] = u_last[0] + pair_update(0, far, SHARED[2])
        arrived('closing 1', 0.25)
        for h in range(2):
            to_sib(1, 2, h, CLOSING[1])
        finish_pair(u_last[0], 0, far)
        finish_pair(u_last[1] + pair_update(1, far, FINAL), 1, far)

    @pl.when(core == 0)
    def _():
        arrived('other shared 2', 0.5)
        u_last[1] = u_last[1] + pair_update(1, far, SHARED[2])
        arrived('final', 0.5)
        finish_pair(u_last[0] + pair_update(0, far, FINAL), 0, far)
        arrived('closing 0', 0.25)
        u_last[1] = u_last[1] + pair_update(1, far, CLOSING[0])
        arrived('closing 1', 0.25)

    for q, slots in enumerate((13, 15)):
        @pl.when(core == q)
        def _():
            everything = bt.at[pl.ds(0, slots)]
            pltpu.make_async_remote_copy(src_ref=everything, dst_ref=everything, send_sem=send_sem, recv_sem=recv_sem.at[0],
                                         device_id={'dap': sib}, device_id_type=MESH).wait_send()


def last_kernel(n_dev, z_buf, a_mat, w_last, u_last, bt_last, out_hbm, cols_buf, sem):
    width = 2 * HALF
    inv_seq = 1.0 / a_mat.shape[0]
    me = lax.axis_index('dap')
    chips = n_dev // 2
    mine = lax.rem(me // 2 + 2, chips) * 2 + 1

    def block(k):
        return pl.ds(pl.multiple_of(lax.rem(mine + k, n_dev) * width, width), width)

    core = lax.rem(me, 2)
    copies = [pltpu.make_async_copy(z_buf.at[:, block(k), :], out_hbm.at[:, block(k), :], sem.at[k]) for k in range(n_dev)]
    for copy in copies[1:]:
        copy.start()

    @pl.when(core == 1)
    def _():
        copies[0].start()

    @pl.when(core == 0)
    def _():
        lhs = [jnp.concatenate([bt_last[h, 0], bt_last[h, 1]], axis=1) for h in range(2)]
        rows = lhs[0].shape[0] * 8
        update = u_last[1] + pair_product(lhs, a_mat, w_last[w_last.shape[0] - rows:, :], inv_seq)
        for h in range(2):
            cols = pl.ds(pl.multiple_of(mine * width + h * HALF, HALF), HALF)
            for g in range(8):
                for k in range(4):
                    i = g * 4 + k
                    part = update[h * BLOCK + g * HALF:h * BLOCK + (g + 1) * HALF, k * LANES:(k + 1) * LANES]
                    cols_buf[i, h * HALF:(h + 1) * HALF, :] = (z_buf[i, cols, :].astype(F32) + part).astype(BF16)
        pltpu.make_async_copy(cols_buf, out_hbm.at[:, block(0), :], sem.at[0]).start()

    for copy in copies:
        copy.wait()


def solution(mesh):
    row_spec = P(('batch', 'dap'))
    col_spec = P(None, ('batch', 'dap'))
    rep_spec = P()
    n_dev = mesh.shape['dap']

    def local_update(z_rows, msa, ln_scale, ln_offset, w_a, b_a, w_b, b_b, w_out, b_out):
        n_seq, n_loc, m_dim = msa.shape
        hid = w_a.shape[1]
        pair = z_rows.shape[2]
        x = jnp.transpose(msa, (1, 2, 0)).reshape(n_loc * m_dim, n_seq)
        any_spec = pl.BlockSpec(memory_space=pltpu.HBM)
        vmem = pltpu.VMEM
        dma = pltpu.SemaphoreType.DMA
        outs = [
            vmem(z_rows.shape, BF16), vmem((n_seq, n_loc * hid), BF16), vmem((8 * LANES, 4 * pair), BF16),
            vmem((2, 2 * BLOCK, 4 * pair), F32), vmem((2, 2, BLOCK // 2, n_seq // 2), BF16),
        ]
        vmem_spec = pl.BlockSpec(memory_space=pltpu.VMEM)
        made = pl.pallas_call(
            functools.partial(kernel, n_dev),
            out_shape=outs,
            in_specs=[any_spec] * 10,
            out_specs=[vmem_spec] * len(outs),
            scratch_shapes=[
                vmem(x.shape, BF16),
                vmem((m_dim,), BF16), vmem((m_dim,), BF16),
                vmem((hid, m_dim), BF16), vmem((hid,), BF16), vmem((hid, m_dim), BF16), vmem((hid,), BF16),
                vmem(w_out.shape, BF16), vmem((pair,), BF16),
                vmem((m_dim, LANES), F32), vmem((m_dim, LANES), F32),
                vmem((4 * hid, LANES), F32), vmem((8 * hid, LANES), F32), vmem((hid, LANES), F32),
                vmem((4 * hid, 4 * m_dim), BF16), vmem((8 * hid, 8 * m_dim), BF16),
                vmem((16, 2, PIECES * BLOCK, n_seq // 2), BF16),
                vmem((PIECES, LANES, 8 * LANES), BF16),
                vmem(w_out.shape, F32), vmem((PIECES - 1, 8 * LANES, 4 * pair), BF16),
                dma((8,)), dma((8,)), dma, dma((17,)), dma,
            ],
            compiler_params=pltpu.CompilerParams(collective_id=0, has_side_effects=True, vmem_limit_bytes=54 * 1024 * 1024),
            name='outer_mean_ring',
        )(*[pltpu.with_memory_space_constraint(part, pltpu.HBM)
            for part in (z_rows, x, ln_scale, ln_offset, w_a.T, b_a, w_b.T, b_b, w_out, b_out)])
        made = [pltpu.with_memory_space_constraint(part, pltpu.VMEM) for part in made]
        return pl.pallas_call(
            functools.partial(last_kernel, n_dev),
            out_shape=jax.ShapeDtypeStruct(z_rows.shape, BF16),
            in_specs=[vmem_spec] * len(outs),
            out_specs=any_spec,
            scratch_shapes=[vmem((n_loc, 2 * HALF, pair), BF16), dma((n_dev,))],
            compiler_params=pltpu.CompilerParams(vmem_limit_bytes=8 * 1024 * 1024),
            name='outer_mean_last',
        )(*made)

    return jax.shard_map(local_update, mesh=mesh, in_specs=(row_spec, col_spec) + (rep_spec,) * 8, out_specs=row_spec, check_vma=False)
```

```python
import functools

import jax
import jax.numpy as jnp
from jax import lax
from jax.experimental import pallas as pl
from jax.experimental.pallas import tpu as pltpu
from jax.sharding import PartitionSpec as P

LN_EPS = 1e-5
F32 = jnp.float32
BF16 = jnp.bfloat16
LANES = 128
HALF = 16
PIECES = 4
BLOCK = 128
ALL = ('rows', 0, 4)
FIRST_OWN = (('lanes', 0, 128), ('lanes', 128, 256), ('lanes', 256, 512))
SECOND_OWN = (('rows', 0, 2), ('rows', 2, 4))
SHARED = (('rows', 0, 1), ('rows', 1, 2), ('rows', 2, 3))
FINAL = ('rows', 3, 4)
CLOSING = (('rows', 3, 3.75), ('rows', 3.75, 4))
MESH = pl.DeviceIdType.MESH


def iota(shape, dim):
    return lax.broadcasted_iota(jnp.int32, shape, dim)


def column_lanes(row, count):
    spread = jnp.broadcast_to(row, (count, count))
    picked = jnp.where(iota((count, count), 0) == iota((count, count), 1), spread, 0.0)
    return jnp.broadcast_to(jnp.sum(picked, axis=1, keepdims=True), (count, LANES))


def pair_product(lhs, a_mat, w_part, inv_seq):
    res = jnp.dot(jnp.concatenate(lhs, axis=0), a_mat[...], preferred_element_type=F32)
    res = (res * inv_seq).astype(BF16)
    size = lhs[0].shape[0]
    wide = jnp.concatenate(
        [jnp.concatenate([res[at:at + HALF, g * LANES:(g + 1) * LANES] for at in range(h * size, (h + 1) * size, HALF)], axis=1)
         for h in range(2) for g in range(8)], axis=0)
    return jnp.dot(wide, w_part, preferred_element_type=F32)


def kernel(n_dev, z_hbm, x_hbm, ls_hbm, lo_hbm, wa_hbm, ba_hbm, wb_hbm, bb_hbm, wo_hbm, bo_hbm,
           z_buf, a_mat, w_last, u_last, bt_last,
           x_buf, ls_v, lo_v, wa_v, ba_v, wb_v, bb_v, wo_v, bo_v,
           scale_bc, offset_bc, bias_a, bias_b, row_bc, proj_a_w, proj_b_w, bt, o_mat, w_f32, w_diag,
           small_sem, x_sem, z_sem, recv_sem, send_sem):
    n_seq = x_hbm.shape[1]
    n_loc = z_hbm.shape[0]
    m_dim = wa_hbm.shape[1]
    hid = wa_hbm.shape[0]
    inv_seq = 1.0 / n_seq
    me = lax.axis_index('dap')
    core = lax.rem(me, 2)
    sib = me + 1 - 2 * core
    right = lax.rem(me + 2, n_dev)
    left = lax.rem(me + n_dev - 2, n_dev)

    barrier = pltpu.get_barrier_semaphore()
    for peer in (sib, right, left):
        pl.semaphore_signal(barrier, inc=1, device_id={'dap': peer}, device_id_type=MESH)

    small = [pltpu.make_async_copy(src, dst, small_sem.at[k]) for k, (src, dst) in enumerate((
        (wb_hbm, wb_v), (bb_hbm, bb_v), (ls_hbm, ls_v), (lo_hbm, lo_v), (wa_hbm, wa_v), (ba_hbm, ba_v),
        (wo_hbm, wo_v), (bo_hbm, bo_v)))]
    half_rows = HALF * m_dim
    half_seq = n_seq // 2
    parts = [(slice(k * half_rows // 2, (k + 1) * half_rows // 2), slice(*group[1:]))
             for group in FIRST_OWN for k in range(2)]
    parts += [(slice(half_rows + k * half_rows // 2, half_rows + (k + 1) * half_rows // 2), slice(0, n_seq)) for k in range(2)]
    x_copies = [pltpu.make_async_copy(x_hbm.at[part], x_buf.at[part], x_sem.at[k]) for k, part in enumerate(parts)]
    for copy in small[:4] + x_copies[:6]:
        copy.start()
    z_copy = pltpu.make_async_copy(z_hbm, z_buf, z_sem)

    for copy in x_copies[:2]:
        copy.wait()
    for copy in small[:4]:
        copy.wait()
    row_bc[...] = column_lanes(bb_v[...].astype(F32).reshape(1, hid), hid)
    wb_rows = wb_v[...].astype(F32)
    wb_two = jnp.concatenate([wb_rows, wb_rows], axis=1)
    scale_bc[...] = column_lanes(ls_v[...].astype(F32).reshape(1, m_dim), m_dim)
    offset_bc[...] = column_lanes(lo_v[...].astype(F32).reshape(1, m_dim), m_dim)
    in_eight = iota((8, LANES), 0)
    in_pair = iota((8, LANES), 1) // m_dim
    for d in range(0, hid, 2):
        for t in range(8 * m_dim // LANES):
            part = [jnp.where(in_eight == in_pair + 2 * t, jnp.broadcast_to(wb_two[e:e + 1, :], (8, LANES)), 0.0)
                    for e in (d, d + 1)]
            proj_b_w[d * 8:(d + 2) * 8, t * LANES:(t + 1) * LANES] = jnp.concatenate(part, axis=0).astype(BF16)
        for e in (d, d + 1):
            bias_b[e * 8:(e + 1) * 8, :] = jnp.broadcast_to(row_bc[e:e + 1, :], (8, LANES))

    def norm_part(rows, lanes, unrolled=False):
        width = lanes.stop - lanes.start
        scale = jnp.concatenate([scale_bc[...]] * (width // LANES), axis=1)
        offset = jnp.concatenate([offset_bc[...]] * (width // LANES), axis=1)

        def body(n, carry):
            at = (pl.ds(rows.start + n * m_dim if unrolled else pl.multiple_of(rows.start + n * m_dim, m_dim), m_dim), lanes)
            value = x_buf[at].astype(F32)
            mean = jnp.sum(value, axis=0, keepdims=True) * (1.0 / m_dim)
            centred = value - mean
            var = jnp.sum(centred * centred, axis=0, keepdims=True) * (1.0 / m_dim)
            normed = centred * lax.rsqrt(var + LN_EPS)
            x_buf[at] = (normed * scale + offset).astype(BF16)
            return carry

        if unrolled:
            for n in range((rows.stop - rows.start) // m_dim):
                body(n, 0)
        else:
            lax.fori_loop(0, (rows.stop - rows.start) // m_dim, body, 0, unroll=8)

    def slot_of(q, r, h):
        return q * 8 + r * 2 + h

    def view(q, r, h, group):
        slot = slot_of(q, r, h)
        if group[0] == 'lanes':
            k = group[1] // half_seq
            return bt.at[slot, k, :, pl.ds(group[1] - k * half_seq, group[2] - group[1])]
        if group == ALL:
            return bt.at[slot]
        return bt.at[slot, :, pl.ds(int(group[1] * BLOCK), int((group[2] - group[1]) * BLOCK)), :]

    names = ['own first', 'own second 0', 'own second 1', 'own shared 0', 'own shared 1', 'own shared 2', 'other r0',
             'other first', 'other second 0', 'other second 1', 'other shared 0', 'other shared 1', 'other shared 2', 'final', 'closing 0', 'closing 1']

    def semaphore_name(mine, r, h, group):
        if group == FINAL:
            return 'final'
        if group in CLOSING:
            return f'closing {CLOSING.index(group)}'
        if r == 2:
            return ('own' if mine else 'other') + f' shared {SHARED.index(group)}'
        if not mine:
            if r == 0:
                return 'other r0'
            return f'other second {SECOND_OWN.index(group)}' if h else 'other first'
        return f'own second {SECOND_OWN.index(group)}' if h else 'own first'

    def transfer(src, dst, name, peer):
        return pltpu.make_async_remote_copy(
            src_ref=src, dst_ref=dst, send_sem=send_sem, recv_sem=recv_sem.at[names.index(name)], device_id={'dap': peer},
            device_id_type=MESH)

    def arrived(name, halves):
        if halves >= 1:
            shape = bt.at[pl.ds(0, halves)]
        else:
            shape = bt.at[pl.ds(0, 2), :, pl.ds(0, int(halves * PIECES * BLOCK) // 2)]
        transfer(shape, shape, name, sib).wait_recv()

    def to_right(q, r, h, group, mine=True):
        there = (r + 3) % 4
        transfer(view(q, r, h, group), view(q, there, h, group), semaphore_name(mine, there, h, group), right).start()

    def to_left(q, r, h, group, mine=True):
        there = (r + 1) % 4
        transfer(view(q, r, h, group), view(q, there, h, group), semaphore_name(mine, there, h, group), left).start()

    def to_sib(q, r, h, group):
        dst = bt_last.at[h] if group == CLOSING[1] else view(q, r, h, group)
        transfer(view(q, r, h, group), dst, semaphore_name(False, r, h, group), sib).start()

    own, other = core, 1 - core

    def project_b(h, lanes):
        width = lanes.stop - lanes.start
        bias = jnp.concatenate([bias_b[...]] * (width // LANES), axis=1)
        res = [jnp.dot(proj_b_w[...], x_buf[h * half_rows + k * half_rows // 2:h * half_rows + (k + 1) * half_rows // 2, lanes],
                       preferred_element_type=F32) + bias for k in range(2)]
        for d in range(hid):
            rows = jnp.concatenate([part[d * 8:(d + 1) * 8, :] for part in res], axis=0).astype(BF16)
            for at in range(lanes.start, lanes.stop, LANES):
                k = at // half_seq
                bt[slot_of(own, 0, h), k, d * HALF:(d + 1) * HALF, at - k * half_seq:at - k * half_seq + LANES] = (
                    rows[:, at - lanes.start:at - lanes.start + LANES])

    for p, group in enumerate(FIRST_OWN):
        for k in range(2):
            if p > 0:
                x_copies[2 * p + k].wait()
            norm_part(*parts[2 * p + k], unrolled=p == 0)
        if p == 1:
            for copy in x_copies[6:] + small[4:] + [z_copy]:
                copy.start()
        project_b(0, parts[2 * p][1])
        if p == 0:
            pl.semaphore_wait(barrier, 3)
        to_right(own, 0, 0, group)
        to_left(own, 0, 0, group)
    to_sib(own, 0, 0, ALL)
    for k in range(2):
        x_copies[6 + k].wait()
        norm_part(*parts[6 + k])
    project_b(1, parts[6][1])
    for group in SECOND_OWN:
        to_right(own, 0, 1, group)
        to_left(own, 0, 1, group)
    to_sib(own, 0, 1, ALL)

    for copy in small[4:]:
        copy.wait()
    row_bc[...] = column_lanes(ba_v[...].astype(F32).reshape(1, hid), hid)
    bias_a[...] = jnp.concatenate([row_bc[...]] * 4, axis=0)
    wa_rows = wa_v[...].astype(F32)
    wa_wide = jnp.concatenate([jnp.concatenate([wa_rows] * 4, axis=1)] * 4, axis=0)
    same = (iota(wa_wide.shape, 0) // hid) == (iota(wa_wide.shape, 1) // m_dim)
    proj_a_w[...] = jnp.where(same, wa_wide, 0.0).astype(BF16)
    for g in range(n_loc // 4):
        res = jnp.dot(proj_a_w[...], x_buf[g * 4 * m_dim:(g + 1) * 4 * m_dim, :], preferred_element_type=F32)
        res = res + jnp.concatenate([bias_a[...]] * (n_seq // LANES), axis=1)
        a_mat[:, g * LANES:(g + 1) * LANES] = res.T.astype(BF16)

    w_f32[...] = wo_v[...].astype(F32)
    w_diag[...] = jnp.zeros_like(w_diag)
    w_last[...] = jnp.zeros_like(w_last)

    def spread_w(d, at):
        block = w_f32[pl.ds(d, hid, stride=hid), :].astype(BF16)
        for k in range(4):
            row = pl.multiple_of(lax.rem(d, 8) * LANES + k * hid, hid)
            at[pl.ds(row, hid), k * LANES:(k + 1) * LANES] = block

    for c in range(PIECES):
        at = w_diag.at[c] if c < PIECES - 1 else w_last

        def body(d, carry):
            spread_w(d, at)
            return carry

        lax.fori_loop(c * 8, (c + 1) * 8, body, 0)

    def outer_piece(slot, c):
        rows = slice(c * BLOCK, (c + 1) * BLOCK)
        lhs = jnp.concatenate([bt[slot, 0, rows, :], bt[slot, 1, rows, :]], axis=1)
        res = jnp.dot(lhs, a_mat[...], preferred_element_type=F32)
        res = (res * inv_seq).astype(BF16)
        for d in range(8):
            for g in range(8):
                o_mat[c, g * HALF:(g + 1) * HALF, d * LANES:(d + 1) * LANES] = (
                    res[d * HALF:(d + 1) * HALF, g * LANES:(g + 1) * LANES])

    def project_piece(c):
        return jnp.dot(o_mat[c], w_diag[c] if c < PIECES - 1 else w_last[...], preferred_element_type=F32)

    chip = me // 2

    def column_of(q, r, h):
        src = lax.rem(chip + r, n_dev // 2) * 2 + q
        return pl.multiple_of(src * (2 * HALF) + h * HALF, HALF)

    bias_out = bo_v[...].astype(F32).reshape(1, LANES)

    def finish(update, bias, q, r, h):
        cols = pl.ds(column_of(q, r, h), HALF)
        for g in range(8):
            for k in range(4):
                i = g * 4 + k
                part = update[g * HALF:(g + 1) * HALF, k * LANES:(k + 1) * LANES]
                if bias is not None:
                    part = part + bias
                z_buf[i, cols, :] = (z_buf[i, cols, :].astype(F32) + part).astype(BF16)

    def half_unit(q, r, h):
        slot = slot_of(q, r, h)
        for c in range(PIECES):
            outer_piece(slot, c)
        update = project_piece(0)
        for c in range(1, PIECES):
            update = update + project_piece(c)
        finish(update, bias_out, q, r, h)

    z_copy.wait()
    for h in range(2):
        half_unit(own, 0, h)
    arrived('other r0', 2)
    for h in range(2):
        half_unit(other, 0, h)
    def pair_update(q, slots, group):
        rows = slice(int(group[1] * BLOCK), int(group[2] * BLOCK))
        lhs = [jnp.concatenate([bt[slot_of(q, r, h), k, rows, :] for k in range(2)], axis=1) for r, h in slots]
        c = int(group[1])
        at = slice(int((group[1] - c) * 8 * LANES), int((group[2] - c) * 8 * LANES))
        return pair_product(lhs, a_mat, w_diag[c, at, :] if c < PIECES - 1 else w_last[at, :], inv_seq)

    def finish_pair(update, q, slots):
        for k, (r, h) in enumerate(slots):
            finish(update[k * BLOCK:(k + 1) * BLOCK, :], None, q, r, h)

    far, near = ((2, 0), (2, 1)), ((3, 1), (1, 1))
    wide_bias = jnp.concatenate([bias_out] * 4, axis=1)

    def send_final(h):
        @pl.when(core == 1)
        def _():
            for q, groups in ((0, (FINAL,)), (1, CLOSING)):
                for group in groups:
                    if h == 0:
                        to_right(q, 3, 0, group)
                    else:
                        to_left(q, 1, 1, group)


    arrived('own first', 2)
    for group in SHARED:
        to_right(own, 3, 0, group)
    for r in (3, 1):
        to_sib(own, r, 0, ALL)
    for r in (3, 1):
        half_unit(own, r, 0)
    arrived('other first', 2)
    send_final(0)
    for r in (3, 1):
        half_unit(other, r, 0)
    for k, group in enumerate(SECOND_OWN):
        arrived(f'own second {k}', 1)
        for part in SHARED:
            if group[1] <= part[1] < group[2]:
                to_left(own, 1, 1, part)
        for r in (3, 1):
            to_sib(own, r, 1, group)
        blocks = [('rows', c, c + 1) for c in range(*group[1:])]
        for q in (own, other):
            if q is other:
                arrived(f'other second {k}', 1)
                if k == 1:
                    send_final(1)
            update = pair_update(q, near, blocks[0]) + pair_update(q, near, blocks[1])
            if k == 0:
                u_last[q] = update + wide_bias
            else:
                finish_pair(u_last[q] + update, q, near)

    for k, group in enumerate(SHARED):
        arrived(f'own shared {k}', 0.5)
        for h in range(2):
            to_sib(own, 2, h, group)
        for q in (own, other)[:2 if k < 2 else 1]:
            if q is other:
                arrived(f'other shared {k}', 0.5)
            update = pair_update(q, far, group)
            u_last[q] = u_last[q] + update if k else update + wide_bias

    @pl.when(core == 1)
    def _():
        arrived('final', 0.5)
        for h in range(2):
            to_sib(0, 2, h, FINAL)
        u_last[0] = u_last[0] + pair_update(0, far, FINAL)
        arrived('closing 0', 0.375)
        for h in range(2):
            to_sib(1, 2, h, CLOSING[0])
        arrived('other shared 2', 0.5)
        u_last[0] = u_last[0] + pair_update(0, far, SHARED[2])
        arrived('closing 1', 0.125)
        for h in range(2):
            to_sib(1, 2, h, CLOSING[1])
        finish_pair(u_last[0], 0, far)
        finish_pair(u_last[1] + pair_update(1, far, FINAL), 1, far)

    @pl.when(core == 0)
    def _():
        arrived('other shared 2', 0.5)
        u_last[1] = u_last[1] + pair_update(1, far, SHARED[2])
        arrived('final', 0.5)
        finish_pair(u_last[0] + pair_update(0, far, FINAL), 0, far)
        arrived('closing 0', 0.375)
        u_last[1] = u_last[1] + pair_update(1, far, CLOSING[0])
        arrived('closing 1', 0.125)

    for q, slots in enumerate((13, 15)):
        @pl.when(core == q)
        def _():
            everything = bt.at[pl.ds(0, slots)]
            pltpu.make_async_remote_copy(src_ref=everything, dst_ref=everything, send_sem=send_sem, recv_sem=recv_sem.at[0],
                                         device_id={'dap': sib}, device_id_type=MESH).wait_send()


def last_kernel(n_dev, z_buf, a_mat, w_last, u_last, bt_last, out_hbm, cols_buf, sem):
    width = 2 * HALF
    inv_seq = 1.0 / a_mat.shape[0]
    me = lax.axis_index('dap')
    chips = n_dev // 2
    mine = lax.rem(me // 2 + 2, chips) * 2 + 1

    def block(k):
        return pl.ds(pl.multiple_of(lax.rem(mine + k, n_dev) * width, width), width)

    core = lax.rem(me, 2)
    copies = [pltpu.make_async_copy(z_buf.at[:, block(k), :], out_hbm.at[:, block(k), :], sem.at[k]) for k in range(n_dev)]
    for copy in copies[1:]:
        copy.start()

    @pl.when(core == 1)
    def _():
        copies[0].start()

    @pl.when(core == 0)
    def _():
        lhs = [jnp.concatenate([bt_last[h, 0], bt_last[h, 1]], axis=1) for h in range(2)]
        rows = lhs[0].shape[0] * 8
        update = u_last[1] + pair_product(lhs, a_mat, w_last[w_last.shape[0] - rows:, :], inv_seq)
        for h in range(2):
            cols = pl.ds(pl.multiple_of(mine * width + h * HALF, HALF), HALF)
            for g in range(8):
                for k in range(4):
                    i = g * 4 + k
                    part = update[h * BLOCK + g * HALF:h * BLOCK + (g + 1) * HALF, k * LANES:(k + 1) * LANES]
                    cols_buf[i, h * HALF:(h + 1) * HALF, :] = (z_buf[i, cols, :].astype(F32) + part).astype(BF16)
        pltpu.make_async_copy(cols_buf, out_hbm.at[:, block(0), :], sem.at[0]).start()

    for copy in copies:
        copy.wait()


def solution(mesh):
    row_spec = P(('batch', 'dap'))
    col_spec = P(None, ('batch', 'dap'))
    rep_spec = P()
    n_dev = mesh.shape['dap']

    def local_update(z_rows, msa, ln_scale, ln_offset, w_a, b_a, w_b, b_b, w_out, b_out):
        n_seq, n_loc, m_dim = msa.shape
        hid = w_a.shape[1]
        pair = z_rows.shape[2]
        x = jnp.transpose(msa, (1, 2, 0)).reshape(n_loc * m_dim, n_seq)
        any_spec = pl.BlockSpec(memory_space=pltpu.HBM)
        vmem = pltpu.VMEM
        dma = pltpu.SemaphoreType.DMA
        outs = [
            vmem(z_rows.shape, BF16), vmem((n_seq, n_loc * hid), BF16), vmem((8 * LANES, 4 * pair), BF16),
            vmem((2, 2 * BLOCK, 4 * pair), F32), vmem((2, 2, BLOCK // 4, n_seq // 2), BF16),
        ]
        vmem_spec = pl.BlockSpec(memory_space=pltpu.VMEM)
        made = pl.pallas_call(
            functools.partial(kernel, n_dev),
            out_shape=outs,
            in_specs=[any_spec] * 10,
            out_specs=[vmem_spec] * len(outs),
            scratch_shapes=[
                vmem(x.shape, BF16),
                vmem((m_dim,), BF16), vmem((m_dim,), BF16),
                vmem((hid, m_dim), BF16), vmem((hid,), BF16), vmem((hid, m_dim), BF16), vmem((hid,), BF16),
                vmem(w_out.shape, BF16), vmem((pair,), BF16),
                vmem((m_dim, LANES), F32), vmem((m_dim, LANES), F32),
                vmem((4 * hid, LANES), F32), vmem((8 * hid, LANES), F32), vmem((hid, LANES), F32),
                vmem((4 * hid, 4 * m_dim), BF16), vmem((8 * hid, 8 * m_dim), BF16),
                vmem((16, 2, PIECES * BLOCK, n_seq // 2), BF16),
                vmem((PIECES, LANES, 8 * LANES), BF16),
                vmem(w_out.shape, F32), vmem((PIECES - 1, 8 * LANES, 4 * pair), BF16),
                dma((8,)), dma((8,)), dma, dma((17,)), dma,
            ],
            compiler_params=pltpu.CompilerParams(collective_id=0, has_side_effects=True, vmem_limit_bytes=54 * 1024 * 1024),
            name='outer_mean_ring',
        )(*[pltpu.with_memory_space_constraint(part, pltpu.HBM)
            for part in (z_rows, x, ln_scale, ln_offset, w_a.T, b_a, w_b.T, b_b, w_out, b_out)])
        made = [pltpu.with_memory_space_constraint(part, pltpu.VMEM) for part in made]
        return pl.pallas_call(
            functools.partial(last_kernel, n_dev),
            out_shape=jax.ShapeDtypeStruct(z_rows.shape, BF16),
            in_specs=[vmem_spec] * len(outs),
            out_specs=any_spec,
            scratch_shapes=[vmem((n_loc, 2 * HALF, pair), BF16), dma((n_dev,))],
            compiler_params=pltpu.CompilerParams(vmem_limit_bytes=8 * 1024 * 1024),
            name='outer_mean_last',
        )(*made)

    return jax.shard_map(local_update, mesh=mesh, in_specs=(row_spec, col_spec) + (rep_spec,) * 8, out_specs=row_spec, check_vma=False)
```
